32 devices in a mesh: gx: 4 (over y, x), gy: 4 (over z), dev: 2 (over core).
Axes of the slice: x: 2, y: 2, z: 4, core: 2. Of those that a mesh axis runs over, the one named last changes fastest.
Arguments:
- fine_now: float32 [3, 8, 64, 1024], P(None, 'dev', 'gx', 'gy'), may hold values from -6 to 6
- fine_before: float32 [3, 8, 64, 1024], P(None, 'dev', 'gx', 'gy'), may hold values from -6 to 6
- fine_material: float32 [4, 8, 64, 1024], P(None, 'dev', 'gx', 'gy'), may hold values from 0.5 to 2
- coarse_now: float32 [3, 16, 32, 512], P(None, 'dev', 'gx', 'gy'), may hold values from -6 to 6
- coarse_before: float32 [3, 16, 32, 512], P(None, 'dev', 'gx', 'gy'), may hold values from -6 to 6
- coarse_material: float32 [3, 16, 32, 512], P(None, 'dev', 'gx', 'gy'), may hold values from 0.5 to 2
Outputs:
- fine_after: float32 [3, 8, 64, 1024], P(None, 'dev', 'gx', 'gy')
- coarse_after: float32 [3, 16, 32, 512], P(None, 'dev', 'gx', 'gy')
The draws below stay inside these ranges and needn't reach their ends.
All inputs are finite; a program needn't handle non-finite values.
Results may differ from the reference program's by a relative error of at most 0.0001.
Values sent between devices are 32-bit elements; how exact they have to be, the bound alone decides.
No kernel may reach another device: no remote copies, remote signals or barrier semaphores. Data moves between devices by JAX's collectives and lax.ppermute only.
A program may use at most 64 MiB of HBM per device.

```python
import math
import jax
import jax.numpy as jnp

STEPS = 2
NXF = 64
NYF = 1024
FZ = 8
NXC = 32
NYC = 512
CZ = 16


def shard_levels(own_key, dims, cuts, smallest, top_value):
    def one(position, parts):
        steps = jax.random.uniform(jax.random.fold_in(jax.random.fold_in(own_key, 6), position), (parts,), jnp.float32, smallest / len(cuts), top_value / len(cuts))
        return jnp.repeat(jnp.exp(steps), dims[position] // parts).reshape((-1,) + (1,) * (len(dims) - position - 1))

    factor_of = one(*cuts[0])
    for cut in cuts[1:]:
        factor_of = factor_of * one(*cut)
    return factor_of


def normal_values(stream_key, extent, deviation, reach, pieces=(), kind=jnp.bfloat16):
    gain = shard_levels(stream_key, extent, pieces, -0.22, 0.18) if pieces else 1.0
    array = jax.random.normal(stream_key, extent, jnp.float32) * deviation * gain
    return jnp.minimum(jnp.maximum(array, -reach), reach).astype(kind)


def setup_inputs(seed: int = 0) -> dict:
    key_list = jax.random.split(jax.random.key(seed), 7)
    return {
        "fine_now": normal_values(key_list[0], (3, FZ, NXF, NYF), 1.0, 6.0, ((1, 2), (2, 4), (3, 4)), jnp.float32),
        "fine_before": normal_values(key_list[1], (3, FZ, NXF, NYF), 1.0, 6.0, ((1, 2), (2, 4), (3, 4)), jnp.float32),
        "fine_material": jnp.clip(jnp.exp(math.log(2.0) - 1.3862944 * jax.random.uniform(key_list[2], (4, FZ, NXF, NYF), jnp.float32) ** shard_levels(key_list[2], (4, FZ, NXF, NYF), ((1, 2), (2, 4), (3, 4)), -0.2, 0.2)), 0.5, 2.0),
        "coarse_now": normal_values(key_list[3], (3, CZ, NXC, NYC), 1.0, 6.0, ((1, 2), (2, 4), (3, 4)), jnp.float32),
        "coarse_before": normal_values(key_list[4], (3, CZ, NXC, NYC), 1.0, 6.0, ((1, 2), (2, 4), (3, 4)), jnp.float32),
        "coarse_material": jnp.clip(jnp.exp(math.log(2.0) - 1.3862944 * jax.random.uniform(key_list[5], (3, CZ, NXC, NYC), jnp.float32) ** shard_levels(key_list[5], (3, CZ, NXC, NYC), ((1, 2), (2, 4), (3, 4)), -0.2, 0.2)), 0.5, 2.0),
    }


time_step = 0.15


def restrict(plane):
    return plane.reshape(plane.shape[0], plane.shape[1] // 2, 2, plane.shape[2] // 2, 2).mean(axis=(2, 4))


def prolong(plane):
    return jnp.repeat(jnp.repeat(plane, 2, axis=1), 2, axis=2)


def backward(field, direction):
    inner = field[1:, 1:, 1:]
    if direction == 0:
        return inner - field[:-1, 1:, 1:]
    if direction == 1:
        return inner - field[1:, :-1, 1:]
    return inner - field[1:, 1:, :-1]


def forces(padded, medium, spacing, stretched):
    centre = padded[:, :-1, :-1, :-1]
    medium_cells = medium[:, :, :-1, :-1]
    if stretched:
        vertical = medium_cells[3] / spacing
        outward = medium[3, 1:, 1:-1, 1:-1] / spacing
    else:
        vertical = 1.0 / spacing
        outward = 1.0 / spacing
    along_z = (padded[:, 1:, :-1, :-1] - centre) * vertical
    along_x = (padded[:, :-1, 1:, :-1] - centre) / spacing
    along_y = (padded[:, :-1, :-1, 1:] - centre) / spacing
    rigidity = medium_cells[1]
    lame_first = medium_cells[2]
    dilation = along_x[0] + along_y[1] + along_z[2]
    normal_x = lame_first * dilation + 2.0 * rigidity * along_x[0]
    normal_y = lame_first * dilation + 2.0 * rigidity * along_y[1]
    normal_z = lame_first * dilation + 2.0 * rigidity * along_z[2]
    shear_xy = rigidity * (along_y[0] + along_x[1])
    shear_xz = rigidity * (along_z[0] + along_x[2])
    shear_yz = rigidity * (along_z[1] + along_y[2])
    force_x = (backward(normal_x, 1) + backward(shear_xy, 2)) / spacing + backward(shear_xz, 0) * outward
    force_y = (backward(shear_xy, 1) + backward(normal_y, 2)) / spacing + backward(shear_yz, 0) * outward
    force_z = (backward(shear_xz, 1) + backward(shear_yz, 2)) / spacing + backward(normal_z, 0) * outward
    return jnp.stack([force_x, force_y, force_z])


def advance(field, before, padded, medium, density, spacing, stretched):
    return 2.0 * field - before + (time_step * time_step) * forces(padded, medium, spacing, stretched) / density


def pad_sides(field):
    return jnp.pad(field, ((0, 0), (0, 0), (1, 1), (1, 1)))


def reference(fine_now, fine_before, fine_material, coarse_now, coarse_before, coarse_material):
    fine_medium = pad_sides(jnp.concatenate([jnp.zeros_like(fine_material[:, :1]), fine_material], axis=1))
    coarse_medium = pad_sides(jnp.concatenate([coarse_material[:, :1], coarse_material], axis=1))
    for instant in range(STEPS):
        fine_ghost = prolong(coarse_now[:, 0])
        coarse_ghost = restrict(fine_now[:, -1])
        fine_padded = pad_sides(jnp.concatenate([jnp.zeros_like(fine_now[:, :1]), fine_now, fine_ghost[:, None]], axis=1))
        coarse_padded = pad_sides(jnp.concatenate([coarse_ghost[:, None], coarse_now, jnp.zeros_like(coarse_now[:, :1])], axis=1))
        fine_next = advance(fine_now, fine_before, fine_padded, fine_medium, fine_material[0], 1.0, True)
        coarse_next = advance(coarse_now, coarse_before, coarse_padded, coarse_medium, coarse_material[0], 2.0, False)
        fine_before, fine_now = fine_now, fine_next
        coarse_before, coarse_now = coarse_now, coarse_next
    return fine_now, coarse_now
```

```python
import functools

import jax
import jax.numpy as jnp
from jax import lax
from jax.experimental import pallas as pl
from jax.experimental.pallas import tpu as pltpu
from jax.sharding import PartitionSpec as P

time_step = 0.15
LANES = 128
MARGIN = 8
U, Q, RHO, MU, LAM, W = 0, 3, 6, 7, 8, 9
FINE_FIELDS, COARSE_FIELDS = 10, 9


def fine_widths(field, layer, layers):
    bottom, above = layer == layers - 1, layer == layers - 2
    if field < Q:
        return (4 if bottom else 3 if above else 2), 2
    if field <= RHO:
        return (2 if bottom else 1), 1
    return (2 if bottom or above else 1), 2


def coarse_widths(field):
    if field < Q:
        return 2, 2
    if field <= RHO:
        return 1, 1
    return 1, 2


def plane_table(fields, layers, widths):
    table, offset = [], 0
    for layer in range(layers):
        for field in range(fields):
            high, low = widths(field, layer)
            table.append((field, layer, high, low, offset))
            offset += max(high, low)
    return table, offset


def round_up(value, multiple):
    return -(-value // multiple) * multiple


def tables(fine_layers, coarse_layers):
    fine, fine_rows = plane_table(
        FINE_FIELDS, fine_layers, lambda f, l: fine_widths(f, l, fine_layers)
    )
    coarse, coarse_rows = plane_table(COARSE_FIELDS, coarse_layers, lambda f, l: coarse_widths(f))
    assert fine_rows <= LANES and coarse_rows <= LANES
    return fine, round_up(fine_rows, 8), coarse, round_up(coarse_rows, 8)


def plane_of(now, before, material, field):
    if field < Q:
        return now, field
    if field < RHO:
        return before, field - Q
    return material, field - RHO


def pack_x_kernel(fu, fp, fm, cu, cp, cm, to_even, to_odd):
    fine, fine_rows, coarse, _ = tables(fu.shape[1], cu.shape[1])
    tiles = fu.shape[3] // LANES
    coarse_tiles = cu.shape[3] // LANES

    def fill(out, first):
        for group, refs, base, rows, parts in (
            (fine, (fu, fp, fm), 0, fine_rows, tiles),
            (coarse, (cu, cp, cm), tiles * fine_rows, tables(fu.shape[1], cu.shape[1])[3], coarse_tiles),
        ):
            for field, layer, high, low, offset in group:
                ref, comp = plane_of(*refs, field)
                size = high if first else low
                start = 0 if first else ref.shape[2] - low
                for t in range(parts):
                    at = base + t * rows + offset
                    out[at : at + size, :] = ref[
                        comp, layer, start : start + size, t * LANES : (t + 1) * LANES
                    ]

    even = lax.rem(lax.axis_index("gx"), 2) == 0

    @pl.when(even)
    def _():
        fill(to_even, False)
        fill(to_odd, True)

    @pl.when(jnp.logical_not(even))
    def _():
        fill(to_even, True)
        fill(to_odd, False)


def pack_y_kernel(fu, fp, fm, cu, cp, cm, got_even, got_odd, fine_out, coarse_out, to_even, to_odd):
    fine, fine_rows, coarse, coarse_rows = tables(fu.shape[1], cu.shape[1])
    tiles = fu.shape[3] // LANES
    coarse_tiles = cu.shape[3] // LANES
    groups = (
        (fine, (fu, fp, fm), fine_out, 0, fine_rows, tiles),
        (coarse, (cu, cp, cm), coarse_out, tiles * fine_rows, coarse_rows, coarse_tiles),
    )

    def halo(high_ref, low_ref):
        for group, refs, out, base, rows, parts in groups:
            for field, layer, high, low, offset in group:
                cells = out.shape[2] - MARGIN
                for t in range(parts):
                    at = base + t * rows + offset
                    lanes = slice(t * LANES, (t + 1) * LANES)
                    out[field, layer, cells : cells + high, lanes] = high_ref[at : at + high, :]
                    out[field, layer, cells + MARGIN - low : cells + MARGIN, lanes] = low_ref[
                        at : at + low, :
                    ]

    for group, refs, out, base, rows, parts in groups:
        for field, layer, high, low, offset in group:
            cells = out.shape[2] - MARGIN
            ref, comp = plane_of(*refs, field)
            out[field, layer, :cells, :] = ref[comp, layer]
            out[field, layer, cells:, :] = jnp.zeros((MARGIN, out.shape[3]), jnp.float32)

    even = lax.rem(lax.axis_index("gx"), 2) == 0

    @pl.when(even)
    def _():
        halo(got_even, got_odd)

    @pl.when(jnp.logical_not(even))
    def _():
        halo(got_odd, got_even)

    packed = []
    for group, refs, out, base, rows, parts in groups:
        shape = (out.shape[2], LANES)
        lane = lax.broadcasted_iota(jnp.int32, shape, 1)
        firsts = jnp.zeros(shape, jnp.float32)
        lasts = jnp.zeros(shape, jnp.float32)
        for field, layer, high, low, offset in group:
            first = out[field, layer, :, :LANES]
            last = out[field, layer, :, out.shape[3] - LANES :]
            first = pltpu.roll(first, offset, 1) if offset else first
            last = pltpu.roll(last, (offset + low) % LANES, 1)
            firsts = jnp.where((lane >= offset) & (lane < offset + high), first, firsts)
            lasts = jnp.where((lane >= offset) & (lane < offset + low), last, lasts)
        packed.append((firsts, lasts))
    fine_height = fine_out.shape[2]
    even_y = lax.rem(lax.axis_index("gy"), 2) == 0

    @pl.when(even_y)
    def _():
        for k, (firsts, lasts) in enumerate(packed):
            at = slice(0, fine_height) if k == 0 else slice(fine_height, None)
            to_even[at, :] = lasts
            to_odd[at, :] = firsts

    @pl.when(jnp.logical_not(even_y))
    def _():
        for k, (firsts, lasts) in enumerate(packed):
            at = slice(0, fine_height) if k == 0 else slice(fine_height, None)
            to_even[at, :] = firsts
            to_odd[at, :] = lasts


def ahead(value, axis):
    return pltpu.roll(value, value.shape[axis] - 1, axis)


def behind(value, axis):
    return value - pltpu.roll(value, 1, axis)


def stress_of(here, below, medium, stretched):
    rigidity, lame = medium[0], medium[1]
    dx = [ahead(f, 0) - f for f in here]
    dy = [ahead(f, 1) - f for f in here]
    dz = [b - f for b, f in zip(below, here)]
    if stretched:
        dz = [f * medium[2] for f in dz]
    trace = lame * (dx[0] + dy[1] + dz[2])
    double = rigidity + rigidity
    return (
        trace + double * dx[0],
        trace + double * dy[1],
        trace + double * dz[2],
        rigidity * (dy[0] + dx[1]),
        rigidity * (dz[0] + dx[2]),
        rigidity * (dz[1] + dy[2]),
    )


def force_of(stress, above, outward):
    nx, ny, nz, xy, xz, yz = stress
    up = [xz - above[0], yz - above[1], nz - above[2]]
    if outward is not None:
        up = [f * outward for f in up]
    return (
        behind(nx, 0) + behind(xy, 1) + up[0],
        behind(xy, 0) + behind(ny, 1) + up[1],
        behind(xz, 0) + behind(yz, 1) + up[2],
    )


def vertical(stress):
    return (stress[4], stress[5], stress[2])


def steps_kernel(
    own_f, own_c, far_f, far_c, own_ye, own_yo, far_ye, far_yo, fine_ref, coarse_ref, fs, fn, cs, cn
):
    layers, height, width = own_f.shape[1:]
    clayers, cheight, cwidth = own_c.shape[1:]
    n, nc = height - MARGIN, cheight - MARGIN
    full, cfull = width + LANES, cwidth + LANES
    depth, cdepth = 2 * layers, 2 * clayers
    fine, _, coarse, _ = tables(layers, clayers)
    gx, gy, dev = lax.axis_index("gx"), lax.axis_index("gy"), lax.axis_index("dev")
    nx, ny = lax.axis_size("gx"), lax.axis_size("gy")

    def assemble(high_ref, low_ref, from_f, from_c, half):
        for group, src, dst, top, count in (
            (fine, from_f, fs, 0, layers),
            (coarse, from_c, cs, height, clayers),
        ):
            rows = src.shape[2]
            lane = lax.broadcasted_iota(jnp.int32, (rows, LANES), 1)
            highs, lows = high_ref[top : top + rows, :], low_ref[top : top + rows, :]
            for field, layer, high, low, offset in group:
                side = jnp.where(
                    lane < high, pltpu.roll(highs, (LANES - offset) % LANES, 1), 0.0
                )
                side = jnp.where(
                    lane >= LANES - low, pltpu.roll(lows, LANES - low - offset, 1), side
                )
                at = half * count + layer
                dst[field, at, :, : src.shape[3]] = src[field, layer]
                dst[field, at, :, src.shape[3] :] = side

    even_y = lax.rem(gy, 2) == 0

    @pl.when(even_y)
    def _():
        assemble(own_ye, own_yo, own_f, own_c, dev)
        assemble(far_ye, far_yo, far_f, far_c, 1 - dev)

    @pl.when(jnp.logical_not(even_y))
    def _():
        assemble(own_yo, own_ye, own_f, own_c, dev)
        assemble(far_yo, far_ye, far_f, far_c, 1 - dev)

    def position(size, extent, axis, shape, turn):
        index = lax.broadcasted_iota(jnp.int32, shape, axis)
        return jnp.where(index < turn, index, index - size)

    fx = position(height, n, 0, (height, full), n + 4)
    fy = position(full, width, 1, (height, full), width + 64)
    cx = position(cheight, nc, 0, (cheight, cfull), nc + 4)
    cy = position(cfull, cwidth, 1, (cheight, cfull), cwidth + 64)
    in_domain_f = (
        (fx + gx * n >= 0) & (fx + gx * n < nx * n)
        & (fy + gy * width >= 0) & (fy + gy * width < ny * width)
    )
    in_domain_c = (
        (cx + gx * nc >= 0) & (cx + gx * nc < nx * nc)
        & (cy + gy * cwidth >= 0) & (cy + gy * cwidth < ny * cwidth)
        & (cx >= -1) & (cx <= nc) & (cy >= -1) & (cy <= cwidth)
    )

    def wrap(index, turn, size):
        return jnp.where(index < turn, index, index - size)

    def pairing(fine_size, fine_turn, coarse_size, transpose):
        shape = (coarse_size, fine_size) if transpose else (fine_size, coarse_size)
        f = wrap(lax.broadcasted_iota(jnp.int32, shape, 1 if transpose else 0), fine_turn, fine_size)
        c = lax.broadcasted_iota(jnp.int32, shape, 0 if transpose else 1)
        half = jnp.right_shift(f, 1)
        half = jnp.where(half < 0, half + coarse_size, half)
        return (half == c).astype(jnp.float32)

    dot = functools.partial(
        jnp.dot, precision=lax.Precision.HIGHEST, preferred_element_type=jnp.float32
    )

    def prolong(plane):
        rows = pairing(height, n + 4, cheight, False)
        lanes = pairing(full, width + 64, cfull, True)
        return dot(rows, dot(plane, lanes))

    def restrict(plane):
        rows = pairing(height, n + 4, cheight, True)
        lanes = pairing(full, width + 64, cfull, False)
        return dot(rows, dot(plane, lanes)) * 0.25

    def ghosts(fine_state, coarse_state):
        for k in range(3):
            fine_state[k, depth] = prolong(coarse_state[k, 1])
            coarse_state[k, 0] = restrict(fine_state[k, depth - 1])

    for k in range(3):
        fn[k, depth] = jnp.zeros((height, full), jnp.float32)
        zero = jnp.zeros((cheight, cfull), jnp.float32)
        cn[k, cdepth + 1] = zero

    @pl.loop(0, cdepth)
    def _(g):
        for k in range(3):
            cn[k, g + 1] = cs[k, g]

    for k in range(3):
        fs[k, depth] = prolong(cn[k, 1])
        cn[k, 0] = restrict(fs[k, depth - 1])

    scale = jnp.float32(time_step * time_step)

    def fine_stress(state, g):
        return stress_of(
            [state[k, g] for k in range(3)],
            [state[k, g + 1] for k in range(3)],
            [fs[k, g] for k in (MU, LAM, W)],
            True,
        )

    def coarse_stress(state, g):
        row = jnp.maximum(g, 0)
        return stress_of(
            [state[k, g + 1] for k in range(3)],
            [state[k, g + 2] for k in range(3)],
            [cs[k, row] for k in (MU, LAM)],
            False,
        )

    def first_fine(g, above):
        stress = fine_stress(fs, g)
        force = force_of(stress, above, fs[W, g])
        rate = scale / fs[RHO, g]
        last = (g == depth - 1).astype(jnp.int32)
        keep = in_domain_f & (fx >= -1) & (fx <= n + last) & (fy >= -1) & (fy <= width + last)
        for k in range(3):
            u = fs[k, g]
            fn[k, g] = jnp.where(keep, u + u - fs[Q + k, g] + force[k] * rate, 0.0)
        return vertical(stress)

    nothing = jnp.zeros((height, full), jnp.float32)
    lax.fori_loop(0, depth, first_fine, (nothing, nothing, nothing))

    def first_coarse(g, above):
        stress = coarse_stress(cn, g)
        force = force_of(stress, above, None)
        rate = (0.25 * scale) / cs[RHO, g]
        for k in range(3):
            v = cs[k, g]
            cs[Q + k, g] = jnp.where(
                in_domain_c, v + v - cs[Q + k, g] + force[k] * rate, 0.0
            )
        return vertical(stress)

    lax.fori_loop(0, cdepth, first_coarse, vertical(coarse_stress(cn, -1)))

    @pl.loop(0, cdepth)
    def _(g):
        for k in range(3):
            cn[k, g + 1] = cs[Q + k, g]

    for k in range(3):
        fn[k, depth] = prolong(cn[k, 1])
        cn[k, 0] = restrict(fn[k, depth - 1])

    def second_fine(l, above):
        g = dev * layers + l
        stress = fine_stress(fn, g)
        force = force_of(stress, above, fs[W, g])
        rate = scale / fs[RHO, g]
        for k in range(3):
            u = fn[k, g]
            out = u + u - fs[k, g] + force[k] * rate
            fine_ref[k, l] = out[:n, :width]
        return vertical(stress)

    start = jnp.maximum(dev * layers - 1, 0)
    entry = [jnp.where(dev == 0, 0.0, f) for f in vertical(fine_stress(fn, start))]
    lax.fori_loop(0, layers, second_fine, tuple(entry))

    def second_coarse(l, above):
        g = dev * clayers + l
        stress = coarse_stress(cn, g)
        force = force_of(stress, above, None)
        rate = (0.25 * scale) / cs[RHO, g]
        for k in range(3):
            v = cn[k, g + 1]
            out = v + v - cs[k, g] + force[k] * rate
            coarse_ref[k, l] = out[:nc, :cwidth]
        return vertical(stress)

    lax.fori_loop(0, clayers, second_coarse, vertical(coarse_stress(cn, dev * clayers - 1)))


def partners(count, parity):
    pairs = [(i, ((i + parity) ^ 1) - parity) for i in range(count)]
    return [(i, j) for i, j in pairs if 0 <= j < count]


def swap(value, axis, parity):
    return lax.ppermute(value, axis, partners(lax.axis_size(axis), parity))


def call(kernel, out_shape, operands, scratch=(), flops=0):
    vmem = pl.BlockSpec(memory_space=pltpu.VMEM)
    size = sum(o.size for o in jax.tree.leaves(out_shape)) * 4
    return pl.pallas_call(
        kernel,
        out_shape=out_shape,
        in_specs=[vmem] * len(operands),
        out_specs=[vmem] * len(out_shape),
        scratch_shapes=list(scratch),
        cost_estimate=pl.CostEstimate(flops=flops, bytes_accessed=size, transcendentals=0),
        compiler_params=pltpu.CompilerParams(vmem_limit_bytes=32 * 1024 * 1024),
    )(*operands)


def shape(*dims):
    return jax.ShapeDtypeStruct(dims, jnp.float32)


def per_device(fine_now, fine_before, fine_material, coarse_now, coarse_before, coarse_material):
    inputs = (fine_now, fine_before, fine_material, coarse_now, coarse_before, coarse_material)
    _, layers, n, width = fine_now.shape
    _, clayers, nc, cwidth = coarse_now.shape
    _, fine_rows, _, coarse_rows = tables(layers, clayers)
    rows = (width // LANES) * fine_rows + (cwidth // LANES) * coarse_rows
    height, cheight = n + MARGIN, nc + MARGIN

    edge = shape(rows, LANES)
    to_even, to_odd = call(pack_x_kernel, (edge, edge), inputs)
    got_odd = swap(to_odd, "gx", 1)
    got_even = swap(to_even, "gx", 0)

    side = shape(height + cheight, LANES)
    tiles = (shape(FINE_FIELDS, layers, height, width), shape(COARSE_FIELDS, clayers, cheight, cwidth))
    own_f, own_c, to_even, to_odd = call(
        pack_y_kernel, tiles + (side, side), inputs + (got_even, got_odd)
    )
    own_yo = swap(to_odd, "gy", 1)
    own_ye = swap(to_even, "gy", 0)
    far_f, far_c = swap(own_f, "dev", 0), swap(own_c, "dev", 0)
    far_yo, far_ye = swap(own_yo, "dev", 0), swap(own_ye, "dev", 0)

    full, cfull = width + LANES, cwidth + LANES
    return call(
        steps_kernel,
        (shape(*fine_now.shape), shape(*coarse_now.shape)),
        (own_f, own_c, far_f, far_c, own_ye, own_yo, far_ye, far_yo),
        scratch=(
            pltpu.VMEM((FINE_FIELDS, 2 * layers + 1, height, full), jnp.float32),
            pltpu.VMEM((3, 2 * layers + 1, height, full), jnp.float32),
            pltpu.VMEM((COARSE_FIELDS, 2 * clayers, cheight, cfull), jnp.float32),
            pltpu.VMEM((3, 2 * clayers + 2, cheight, cfull), jnp.float32),
        ),
    )


def solution(mesh):
    spec = P(None, "dev", "gx", "gy")
    return jax.shard_map(
        per_device,
        mesh=mesh,
        in_specs=(spec,) * 6,
        out_specs=(spec, spec),
        check_vma=False,
    )
```

```python
import jax
import jax.numpy as jnp
from jax import lax
from jax.experimental import pallas as pl
from jax.experimental.pallas import tpu as pltpu
from jax.sharding import PartitionSpec as P


time_step = 0.15
LANES = 128
MARGIN = 8
U, Q, RHO, MU, LAM, W = 0, 3, 6, 7, 8, 9
FINE_FIELDS, COARSE_FIELDS = 10, 9


def fine_widths(field, layer, layers):
    bottom, above = layer == layers - 1, layer == layers - 2
    if field < Q:
        return (4 if bottom else 3 if above else 2), 2
    if field <= RHO:
        return (2 if bottom else 1), 1
    return (2 if bottom or above else 1), 2


def coarse_widths(field):
    if field < Q:
        return 2, 2
    if field <= RHO:
        return 1, 1
    return 1, 2


def plane_table(fields, layers, widths):
    table, offset = [], 0
    for layer in range(layers):
        for field in range(fields):
            high, low = widths(field, layer)
            table.append((field, layer, high, low, offset))
            offset += max(high, low)
    return table, offset


def round_up(value, multiple):
    return -(-value // multiple) * multiple


def tables(fine_layers, coarse_layers):
    fine, fine_rows = plane_table(
        FINE_FIELDS, fine_layers, lambda f, l: fine_widths(f, l, fine_layers)
    )
    coarse, coarse_rows = plane_table(COARSE_FIELDS, coarse_layers, lambda f, l: coarse_widths(f))
    assert fine_rows <= LANES and coarse_rows <= LANES
    return fine, round_up(fine_rows, 8), coarse, round_up(coarse_rows, 8)


def groups_of(fine_layers, coarse_layers, fine_parts, coarse_parts):
    fine, fine_rows, coarse, coarse_rows = tables(fine_layers, coarse_layers)
    return (fine, 0, fine_rows, fine_parts), (
        coarse,
        fine_parts * fine_rows,
        coarse_rows,
        coarse_parts,
    )


def pack_x_kernel(fu, fp, fm, cu, cp, cm, fine, coarse, to_even, to_odd, sems):
    copies = []
    for out, sources in ((fine, (fu, fp, fm)), (coarse, (cu, cp, cm))):
        for first, source in zip((U, Q, RHO), sources):
            copies.append(
                pltpu.make_async_copy(
                    source, out.at[first : first + source.shape[0]], sems.at[len(copies)]
                )
            )
    for copy in copies:
        copy.start()
    for copy in copies:
        copy.wait()
    groups = groups_of(
        fine.shape[1], coarse.shape[1], fine.shape[3] // LANES, coarse.shape[3] // LANES
    )

    def fill(out, first):
        for (table, base, rows, parts), ref in zip(groups, (fine, coarse)):
            for field, layer, high, low, offset in table:
                size = high if first else low
                start = 0 if first else ref.shape[2] - low
                for t in range(parts):
                    at = base + t * rows + offset
                    out[at : at + size, :] = ref[
                        field, layer, start : start + size, t * LANES : (t + 1) * LANES
                    ]

    even = lax.rem(lax.axis_index("gx"), 2) == 0

    @pl.when(even)
    def _():
        fill(to_even, False)
        fill(to_odd, True)

    @pl.when(jnp.logical_not(even))
    def _():
        fill(to_even, True)
        fill(to_odd, False)


def pack_y_kernel(fine, coarse, got_even, got_odd, fine_halo, coarse_halo, to_even, to_odd):
    groups = groups_of(
        fine.shape[1], coarse.shape[1], fine.shape[3] // LANES, coarse.shape[3] // LANES
    )

    def halo(high_ref, low_ref):
        for (table, base, rows, parts), out in zip(groups, (fine_halo, coarse_halo)):
            for field, layer, high, low, offset in table:
                for t in range(parts):
                    at = base + t * rows + offset
                    lanes = slice(t * LANES, (t + 1) * LANES)
                    out[field, layer, :high, lanes] = high_ref[at : at + high, :]
                    out[field, layer, MARGIN - low :, lanes] = low_ref[at : at + low, :]

    for (table, *_), out in zip(groups, (fine_halo, coarse_halo)):
        for field, layer, high, low, offset in table:
            out[field, layer] = jnp.zeros((MARGIN, out.shape[3]), jnp.float32)

    even = lax.rem(lax.axis_index("gx"), 2) == 0

    @pl.when(even)
    def _():
        halo(got_even, got_odd)

    @pl.when(jnp.logical_not(even))
    def _():
        halo(got_odd, got_even)

    packed = []
    for (table, *_), ref, edge in zip(groups, (fine, coarse), (fine_halo, coarse_halo)):
        shape = (ref.shape[2] + MARGIN, LANES)
        lane = lax.broadcasted_iota(jnp.int32, shape, 1)
        firsts = jnp.zeros(shape, jnp.float32)
        lasts = jnp.zeros(shape, jnp.float32)
        for field, layer, high, low, offset in table:
            left, right = slice(0, LANES), slice(ref.shape[3] - LANES, ref.shape[3])
            first, last = (
                jnp.concatenate([ref[field, layer, :, s], edge[field, layer, :, s]], axis=0)
                for s in (left, right)
            )
            first = pltpu.roll(first, offset, 1) if offset else first
            last = pltpu.roll(last, (offset + low) % LANES, 1)
            firsts = jnp.where((lane >= offset) & (lane < offset + high), first, firsts)
            lasts = jnp.where((lane >= offset) & (lane < offset + low), last, lasts)
        packed.append((firsts, lasts))
    height = fine.shape[2] + MARGIN
    even_y = lax.rem(lax.axis_index("gy"), 2) == 0

    @pl.when(even_y)
    def _():
        for at, (firsts, lasts) in zip((slice(0, height), slice(height, None)), packed):
            to_even[at, :] = lasts
            to_odd[at, :] = firsts

    @pl.when(jnp.logical_not(even_y))
    def _():
        for at, (firsts, lasts) in zip((slice(0, height), slice(height, None)), packed):
            to_even[at, :] = firsts
            to_odd[at, :] = lasts


def ahead(value, axis):
    return pltpu.roll(value, value.shape[axis] - 1, axis)


def behind(value, axis):
    return value - pltpu.roll(value, 1, axis)


def stress_of(here, below, medium, stretched):
    rigidity, lame = medium[0], medium[1]
    dx = [ahead(f, 0) - f for f in here]
    dy = [ahead(f, 1) - f for f in here]
    dz = [b - f for b, f in zip(below, here)]
    if stretched:
        dz = [f * medium[2] for f in dz]
    trace = lame * (dx[0] + dy[1] + dz[2])
    double = rigidity + rigidity
    return (
        trace + double * dx[0],
        trace + double * dy[1],
        trace + double * dz[2],
        rigidity * (dy[0] + dx[1]),
        rigidity * (dz[0] + dx[2]),
        rigidity * (dz[1] + dy[2]),
    )


def force_of(stress, above, outward):
    nx, ny, nz, xy, xz, yz = stress
    up = [xz, yz, nz]
    if above is not None:
        up = [f - a for f, a in zip(up, (above[4], above[5], above[2]))]
    if outward is not None:
        up = [f * outward for f in up]
    return (
        behind(nx, 0) + behind(xy, 1) + up[0],
        behind(xy, 0) + behind(ny, 1) + up[1],
        behind(xz, 0) + behind(yz, 1) + up[2],
    )


def bf16_parts(value):
    parts = []
    for _ in range(3):
        part = value.astype(jnp.bfloat16)
        parts.append(part)
        value = value - part.astype(jnp.float32)
    return parts


def select_lanes(planes, matrix):
    rows = planes[0].shape[0]
    parts = bf16_parts(jnp.concatenate(planes, axis=0))
    product = jnp.dot(
        jnp.concatenate(parts, axis=0), matrix, preferred_element_type=jnp.float32
    )
    size = rows * len(planes)
    total = product[:size] + product[size : 2 * size] + product[2 * size :]
    return [total[k * rows : (k + 1) * rows] for k in range(len(planes))]


def select_rows(matrix, planes):
    lanes = planes[0].shape[1]
    parts = bf16_parts(jnp.concatenate(planes, axis=1))
    product = jnp.dot(
        jnp.concatenate([matrix] * 3, axis=1),
        jnp.concatenate(parts, axis=0),
        preferred_element_type=jnp.float32,
    )
    return [product[:, k * lanes : (k + 1) * lanes] for k in range(len(planes))]


def bf16_mask(condition):
    return jnp.where(condition, 1.0, 0.0).astype(jnp.bfloat16)


class Grids:
    def __init__(self, height, cheight, lanes, clanes, lane_of):
        def pairs(shape, fine_axis, size_of):
            f = lax.broadcasted_iota(jnp.int32, shape, fine_axis)
            c = lax.broadcasted_iota(jnp.int32, shape, 1 - fine_axis)
            return bf16_mask(size_of(f) == c)

        def row_of(f):
            turn = height - MARGIN // 2
            return jnp.right_shift(jnp.where(f < turn, f, f - height + 2 * cheight), 1)

        self.up_rows = pairs((height, cheight), 0, row_of)
        self.down_rows = pairs((cheight, height), 1, row_of)
        self.up_lanes = pairs((clanes, lanes), 1, lane_of)
        self.down_lanes = pairs((lanes, clanes), 0, lane_of)

    def prolong(self, planes):
        return select_rows(self.up_rows, select_lanes(planes, self.up_lanes))

    def restrict(self, planes):
        planes = select_lanes(select_rows(self.down_rows, planes), self.down_lanes)
        return [0.25 * plane for plane in planes]


def row_index(height, shape):
    index = lax.broadcasted_iota(jnp.int32, shape, 0)
    return jnp.where(index < height - MARGIN // 2, index, index - height)


def two_steps(dev, layers, clayers, fine, coarse, grids, keep_f, keep_c, state_f, state_c, out_f, out_c):
    depth, cdepth = 2 * layers, 2 * clayers
    scale = jnp.float32(time_step * time_step)
    three = range(3)
    ghost_f = grids.prolong([coarse(k, 0) for k in three])
    ghost_c = grids.restrict([fine(k, depth - 1) for k in three])

    def solver(plane, medium, ghost_above, ghost_below, last, stretched, first_layer):
        known = {}

        def here(g):
            if g < 0:
                return ghost_above
            if g == last + 1:
                return ghost_below
            return [plane(k, g) for k in three]

        def stress(g):
            if g < first_layer:
                return None
            if g not in known:
                top = max(g, 0)
                known[g] = stress_of(
                    here(g), here(g + 1), [medium(k, top) for k in (MU, LAM, W)[: 3 if stretched else 2]], stretched
                )
            return known[g]

        return stress

    zero_c = [jnp.zeros_like(ghost_c[0])] * 3
    stress_f = solver(fine, fine, None, ghost_f, depth - 1, True, 0)
    stress_c = solver(coarse, coarse, ghost_c, zero_c, cdepth - 1, False, -1)
    own = range(dev * layers, (dev + 1) * layers)
    cown = range(dev * clayers, (dev + 1) * clayers)
    near = sorted({max(own[0] - 1, 0), *own, min(own[-1] + 1, depth - 1)} | ({depth - 1} if dev == 0 else set()))
    cnear = sorted({0, max(cown[0] - 1, 0), *cown, min(cown[-1] + 1, cdepth - 1)})
    for g in near:
        force = force_of(stress_f(g), stress_f(g - 1), fine(W, g))
        rate = scale / fine(RHO, g)
        for k in three:
            u = fine(k, g)
            state_f[k, g] = jnp.where(keep_f(g), u + u - fine(Q + k, g) + force[k] * rate, 0.0)
    for g in cnear:
        force = force_of(stress_c(g), stress_c(g - 1), None)
        rate = (0.25 * scale) / coarse(RHO, g)
        for k in three:
            v = coarse(k, g)
            state_c[k, g] = jnp.where(keep_c, v + v - coarse(Q + k, g) + force[k] * rate, 0.0)

    ghost_f = ghost_c = None
    if dev == 1:
        ghost_f = grids.prolong([state_c[k, 0] for k in three])
    else:
        ghost_c = grids.restrict([state_f[k, depth - 1] for k in three])
    stress_f = solver(lambda k, g: state_f[k, g], fine, None, ghost_f, depth - 1, True, 0)
    stress_c = solver(lambda k, g: state_c[k, g], coarse, ghost_c, zero_c, cdepth - 1, False, -1)
    for l, g in enumerate(own):
        force = force_of(stress_f(g), stress_f(g - 1), fine(W, g))
        rate = scale / fine(RHO, g)
        for k in three:
            u = state_f[k, g]
            out_f(k, l, u + u - fine(k, g) + force[k] * rate)
    for l, g in enumerate(cown):
        force = force_of(stress_c(g), stress_c(g - 1), None)
        rate = (0.25 * scale) / coarse(RHO, g)
        for k in three:
            v = state_c[k, g]
            out_c(k, l, v + v - coarse(k, g) + force[k] * rate)


def for_each_core(body):
    dev = lax.axis_index("dev")

    @pl.when(dev == 0)
    def _():
        body(0)

    @pl.when(dev != 0)
    def _():
        body(1)


def inside(index, axis, size):
    at = index + lax.axis_index(axis) * size
    return (at >= 0) & (at < lax.axis_size(axis) * size)


def main_kernel(
    own_f, own_c, far_f, far_c, own_fh, own_ch, far_fh, far_ch, out_f, out_c, strip_f, strip_c, state_f, state_c
):
    layers, n, width = own_f.shape[1:]
    clayers, nc, cwidth = own_c.shape[1:]
    height, cheight = n + MARGIN, nc + MARGIN
    fx = row_index(height, (height, width))
    cx = row_index(cheight, (cheight, cwidth))
    rows_f = inside(fx, "gx", n) & (fx >= -1)
    keep_c = inside(cx, "gx", nc) & (cx >= -1) & (cx <= nc)
    grids = Grids(height, cheight, width, cwidth, lambda f: jnp.right_shift(f, 1))

    def body(dev):
        def reader(own, far, own_halo, far_halo, count):
            def read(field, g, lanes=slice(None)):
                mine = g // count == dev
                ref, edge = (own, own_halo) if mine else (far, far_halo)
                return jnp.concatenate(
                    [ref[field, g % count, :, lanes], edge[field, g % count, :, lanes]], axis=0
                )

            return read

        fine = reader(own_f, far_f, own_fh, far_fh, layers)
        coarse = reader(own_c, far_c, own_ch, far_ch, clayers)

        def store_f(k, l, value):
            out_f[k, l] = value[:n]

        def store_c(k, l, value):
            out_c[k, l] = value[:nc]

        two_steps(
            dev, layers, clayers, fine, coarse, grids,
            lambda g: rows_f & (fx <= n + (g == 2 * layers - 1)), keep_c,
            state_f, state_c, store_f, store_c,
        )
        for read, strip, fields, count, room in (
            (fine, strip_f, FINE_FIELDS, layers, 4),
            (coarse, strip_c, COARSE_FIELDS, clayers, 2),
        ):
            lane = lax.broadcasted_iota(jnp.int32, strip.shape[2:], 1)
            wide = own_f.shape[3] if room == 4 else own_c.shape[3]
            for field in range(fields):
                for g in strip_layers(dev, count, room == 4):
                    left = pltpu.roll(read(field, g, slice(0, LANES)), room, 1)
                    right = pltpu.roll(
                        read(field, g, slice(wide - LANES, wide)), LANES - room, 1
                    )
                    strip[field, g] = jnp.where(lane < LANES // 2, left, right)

    for_each_core(body)


def strip_layers(dev, count, fine):
    depth = 2 * count
    if fine:
        return range(depth) if dev == 0 else range(count - 2, depth)
    if dev == 0:
        return range(count + 2)
    return [0, 1, *range(count - 2, depth)]


def strip_kernel(
    strip_f, strip_c, main_f, main_c, own_ye, own_yo, far_ye, far_yo, out_f, out_c, fs, cs, state_f, state_c
):
    layers, n, width = main_f.shape[1:]
    clayers, nc, cwidth = main_c.shape[1:]
    height, cheight = n + MARGIN, nc + MARGIN
    fine_table, _, coarse_table, _ = tables(layers, clayers)
    middle = LANES // 2
    fx = row_index(height, (height, LANES))
    cx = row_index(cheight, (cheight, LANES))
    lane_f = lax.broadcasted_iota(jnp.int32, (height, LANES), 1)
    lane_c = lax.broadcasted_iota(jnp.int32, (cheight, LANES), 1)
    fy = jnp.where(lane_f < middle, lane_f - 4, lane_f - LANES + 4 + width)
    cy = jnp.where(lane_c < middle, lane_c - 2, lane_c - LANES + 2 + cwidth)
    base_f = inside(fx, "gx", n) & inside(fy, "gy", width) & (fx >= -1) & (fy >= -1)
    keep_c = (
        inside(cx, "gx", nc) & inside(cy, "gy", cwidth)
        & (cx >= -1) & (cx <= nc) & (cy >= -1) & (cy <= cwidth)
    )
    grids = Grids(
        height, cheight, LANES, LANES,
        lambda f: jnp.right_shift(f, 1) + jnp.where(f < middle, 0, middle),
    )
    even = lax.rem(lax.axis_index("gy"), 2) == 0

    def body(dev):
        for table, src, dst, top, count, room, lane in (
            (fine_table, strip_f, fs, 0, layers, 4, lane_f),
            (coarse_table, strip_c, cs, height, clayers, 2, lane_c),
        ):
            rows = src.shape[2]
            for near in (True, False):
                e, o = (own_ye, own_yo) if near else (far_ye, far_yo)
                e, o = e[top : top + rows, :], o[top : top + rows, :]
                highs, lows = jnp.where(even, e, o), jnp.where(even, o, e)
                for field, layer, high, low, offset in table:
                    g = (dev if near else 1 - dev) * count + layer
                    if g not in strip_layers(dev, count, room == 4):
                        continue
                    start = LANES - room
                    value = src[field, g]
                    value = jnp.where(
                        (lane >= start) & (lane < start + high),
                        pltpu.roll(highs, (start - offset) % LANES, 1), value,
                    )
                    start = room - low
                    value = jnp.where(
                        (lane >= start) & (lane < start + low),
                        pltpu.roll(lows, (start - offset) % LANES, 1), value,
                    )
                    dst[field, g] = value

        def put(out, main, k, l, value, cells, room):
            wide = out.shape[3]
            lane = lax.broadcasted_iota(jnp.int32, (cells, LANES), 1)
            first = pltpu.roll(value[:cells], LANES - room, 1)
            last = pltpu.roll(value[:cells], room, 1)
            for start in range(0, wide, LANES):
                part = main[k, l, :, start : start + LANES]
                if start == 0:
                    part = jnp.where(lane < room, first, part)
                if start == wide - LANES:
                    part = jnp.where(lane >= LANES - room, last, part)
                out[k, l, :, start : start + LANES] = part

        two_steps(
            dev, layers, clayers,
            lambda field, g: fs[field, g], lambda field, g: cs[field, g], grids,
            lambda g: base_f & (fx <= n + (g == 2 * layers - 1)) & (fy <= width + (g == 2 * layers - 1)),
            keep_c, state_f, state_c,
            lambda k, l, value: put(out_f, main_f, k, l, value, n, 4),
            lambda k, l, value: put(out_c, main_c, k, l, value, nc, 2),
        )

    for_each_core(body)


def partners(count, parity):
    pairs = [(i, ((i + parity) ^ 1) - parity) for i in range(count)]
    return [(i, j) for i, j in pairs if 0 <= j < count]


def swap(value, axis, parity):
    return lax.ppermute(value, axis, partners(lax.axis_size(axis), parity))


def call(kernel, out_shape, operands, scratch=(), flops=0, space=pltpu.VMEM, limit=24):
    size = sum(o.size for o in out_shape) * 4
    call = pl.pallas_call(
        kernel,
        out_shape=out_shape,
        in_specs=[pl.BlockSpec(memory_space=space)] * len(operands),
        out_specs=[pl.BlockSpec(memory_space=pltpu.VMEM)] * len(out_shape),
        scratch_shapes=list(scratch),
        cost_estimate=pl.CostEstimate(flops=flops, bytes_accessed=size, transcendentals=0),
        compiler_params=pltpu.CompilerParams(vmem_limit_bytes=limit * 1024 * 1024),
    )
    if space == pltpu.HBM:
        operands = [pltpu.with_memory_space_constraint(o, space) for o in operands]
    return call(*operands)


def shape(*dims):
    return jax.ShapeDtypeStruct(dims, jnp.float32)


def per_device(*inputs):
    _, layers, n, width = inputs[0].shape
    _, clayers, nc, cwidth = inputs[3].shape
    _, fine_rows, _, coarse_rows = tables(layers, clayers)
    rows = (width // LANES) * fine_rows + (cwidth // LANES) * coarse_rows
    height, cheight = n + MARGIN, nc + MARGIN

    edge = shape(rows, LANES)
    own_f, own_c, to_even, to_odd = call(
        pack_x_kernel,
        (shape(FINE_FIELDS, layers, n, width), shape(COARSE_FIELDS, clayers, nc, cwidth), edge, edge),
        inputs,
        scratch=(pltpu.SemaphoreType.DMA((6,)),),
        space=pltpu.HBM,
        limit=24,
    )
    got_odd = swap(to_odd, "gx", 1)
    got_even = swap(to_even, "gx", 0)
    far_f, far_c = swap(own_f, "dev", 0), swap(own_c, "dev", 0)

    side = shape(height + cheight, LANES)
    own_fh, own_ch, to_even, to_odd = call(
        pack_y_kernel,
        (
            shape(FINE_FIELDS, layers, MARGIN, width),
            shape(COARSE_FIELDS, clayers, MARGIN, cwidth),
            side,
            side,
        ),
        (own_f, own_c, got_even, got_odd),
    )
    own_yo = swap(to_odd, "gy", 1)
    own_ye = swap(to_even, "gy", 0)
    far_fh, far_ch = swap(own_fh, "dev", 0), swap(own_ch, "dev", 0)

    def states(lanes, clanes):
        return (
            pltpu.VMEM((3, 2 * layers, height, lanes), jnp.float32),
            pltpu.VMEM((3, 2 * clayers, cheight, clanes), jnp.float32),
        )

    results = (shape(*inputs[0].shape), shape(*inputs[3].shape))
    strips = (
        (FINE_FIELDS, 2 * layers, height, LANES),
        (COARSE_FIELDS, 2 * clayers, cheight, LANES),
    )
    main_f, main_c, strip_f, strip_c = call(
        main_kernel,
        results + tuple(shape(*dims) for dims in strips),
        (own_f, own_c, far_f, far_c, own_fh, own_ch, far_fh, far_ch),
        scratch=states(width, cwidth),
        flops=MAIN_FLOPS,
    )
    far_yo, far_ye = swap(own_yo, "dev", 0), swap(own_ye, "dev", 0)
    return call(
        strip_kernel,
        results,
        (strip_f, strip_c, main_f, main_c, own_ye, own_yo, far_ye, far_yo),
        scratch=tuple(pltpu.VMEM(dims, jnp.float32) for dims in strips) + states(LANES, LANES),
    )


MAIN_FLOPS = 4_000_000


def solution(mesh):
    spec = P(None, "dev", "gx", "gy")

    return jax.shard_map(
        per_device,
        mesh=mesh,
        in_specs=(spec,) * 6,
        out_specs=(spec, spec),
        check_vma=False,
    )
```

```python
import functools

import jax
import jax.numpy as jnp
from jax import lax
from jax.experimental import pallas as pl
from jax.experimental.pallas import tpu as pltpu
from jax.sharding import PartitionSpec as P


time_step = 0.15
LANES = 128
MARGIN = 8
U, Q, RHO, MU, LAM, W = 0, 3, 6, 7, 8, 9
FINE_FIELDS, COARSE_FIELDS = 10, 9


def fine_widths(field, layer, layers):
    bottom, above = layer == layers - 1, layer == layers - 2
    if field < Q:
        return (4 if bottom else 3 if above else 2), 2
    if field <= RHO:
        return (2 if bottom else 1), 1
    return (2 if bottom or above else 1), 2


def coarse_widths(field):
    if field < Q:
        return 2, 2
    if field <= RHO:
        return 1, 1
    return 1, 2


def plane_table(fields, layers, widths):
    table, offset = [], 0
    for layer in range(layers):
        for field in range(fields):
            high, low = widths(field, layer)
            table.append((field, layer, high, low, offset))
            offset += max(high, low)
    return table, offset


def round_up(value, multiple):
    return -(-value // multiple) * multiple


def tables(fine_layers, coarse_layers):
    fine, fine_lanes = plane_table(
        FINE_FIELDS, fine_layers, lambda f, l: fine_widths(f, l, fine_layers)
    )
    coarse, coarse_lanes = plane_table(COARSE_FIELDS, coarse_layers, lambda f, l: coarse_widths(f))
    assert fine_lanes <= LANES and coarse_lanes <= LANES
    return fine, coarse


def edge_rows(tables_of_grids, parts_of_grids, first):
    pieces, at = [], 0
    for grid, (table, parts) in enumerate(zip(tables_of_grids, parts_of_grids)):
        for field, layer, high, low, _ in table:
            size = high if first else low
            for t in range(parts):
                pieces.append((grid, field, layer, t, size, at))
                at += size
    return pieces, round_up(at, 8)


def grid_tables(fine_shape, coarse_shape):
    fine, coarse = tables(fine_shape[1], coarse_shape[1])
    return (fine, coarse), (fine_shape[3] // LANES, coarse_shape[3] // LANES)


def pack_x_kernel(fu, fp, fm, cu, cp, cm, fine, coarse, to_even, to_odd, sems):
    copies = []
    for out, sources in ((fine, (fu, fp, fm)), (coarse, (cu, cp, cm))):
        for first, source in zip((U, Q, RHO), sources):
            copies.append(
                pltpu.make_async_copy(
                    source, out.at[first : first + source.shape[0]], sems.at[len(copies)]
                )
            )
    for copy in copies:
        copy.start()
    for copy in copies:
        copy.wait()
    grids = grid_tables(fine.shape, coarse.shape)

    def fill(out, first):
        for grid, field, layer, t, size, at in edge_rows(*grids, first)[0]:
            ref = (fine, coarse)[grid]
            start = 0 if first else ref.shape[2] - size
            out[at : at + size, :] = ref[
                field, layer, start : start + size, t * LANES : (t + 1) * LANES
            ]

    even = lax.rem(lax.axis_index("gx"), 2) == 0

    @pl.when(even)
    def _():
        fill(to_even, False)
        fill(to_odd, True)

    @pl.when(jnp.logical_not(even))
    def _():
        fill(to_even, True)
        fill(to_odd, False)


def edge_columns(table, read, height, width):
    lane = lax.broadcasted_iota(jnp.int32, (height, LANES), 1)
    firsts = jnp.zeros((height, LANES), jnp.float32)
    lasts = jnp.zeros((height, LANES), jnp.float32)
    for field, layer, high, low, offset in table:
        first = read(field, layer, slice(0, LANES))
        last = read(field, layer, slice(width - LANES, width))
        first = pltpu.roll(first, offset, 1) if offset else first
        last = pltpu.roll(last, (offset + low) % LANES, 1)
        firsts = jnp.where((lane >= offset) & (lane < offset + high), first, firsts)
        lasts = jnp.where((lane >= offset) & (lane < offset + low), last, lasts)
    return firsts, lasts


def pack_inner_kernel(fine, coarse, firsts_ref, lasts_ref):
    at = 0
    for table, ref in zip(grid_tables(fine.shape, coarse.shape)[0], (fine, coarse)):
        rows = ref.shape[2]
        firsts, lasts = edge_columns(
            table, lambda field, layer, lanes: ref[field, layer, :, lanes], rows, ref.shape[3]
        )
        firsts_ref[at : at + rows, :] = firsts
        lasts_ref[at : at + rows, :] = lasts
        at += rows


def pack_y_kernel(fine_rows, firsts_ref, lasts_ref, got_even, got_odd, fine_halo, coarse_halo, to_even, to_odd):
    halos = (fine_halo, coarse_halo)
    grids = grid_tables(fine_halo.shape, coarse_halo.shape)

    def halo(high_ref, low_ref):
        for first, ref in ((True, high_ref), (False, low_ref)):
            for grid, field, layer, t, size, at in edge_rows(*grids, first)[0]:
                start = 0 if first else MARGIN - size
                halos[grid][field, layer, start : start + size, t * LANES : (t + 1) * LANES] = ref[
                    at : at + size, :
                ]

    for table, out in zip(grids[0], halos):
        for field, layer, *_ in table:
            out[field, layer] = jnp.zeros((MARGIN, out.shape[3]), jnp.float32)

    even = lax.rem(lax.axis_index("gx"), 2) == 0

    @pl.when(even)
    def _():
        halo(got_even, got_odd)

    @pl.when(jnp.logical_not(even))
    def _():
        halo(got_odd, got_even)

    columns = [
        edge_columns(
            table, lambda field, layer, lanes: out[field, layer, :, lanes], MARGIN, out.shape[3]
        )
        for table, out in zip(grids[0], halos)
    ]
    even_y = lax.rem(lax.axis_index("gy"), 2) == 0

    def place(first_out, last_out):
        for side, (inner, out) in enumerate(((firsts_ref, first_out), (lasts_ref, last_out))):
            pieces = [
                inner[:fine_rows, :],
                columns[0][side],
                inner[fine_rows:, :],
                columns[1][side],
            ]
            at = 0
            for piece in pieces:
                out[at : at + piece.shape[0], :] = piece
                at += piece.shape[0]

    @pl.when(even_y)
    def _():
        place(to_odd, to_even)

    @pl.when(jnp.logical_not(even_y))
    def _():
        place(to_even, to_odd)


def ahead(value, axis):
    return pltpu.roll(value, value.shape[axis] - 1, axis)


def behind(value, axis):
    return value - pltpu.roll(value, 1, axis)


def stress_of(here, below, medium, stretched):
    rigidity, lame = medium[0], medium[1]
    dx = [ahead(f, 0) - f for f in here]
    dy = [ahead(f, 1) - f for f in here]
    dz = [b - f for b, f in zip(below, here)]
    if stretched:
        dz = [f * medium[2] for f in dz]
    trace = lame * (dx[0] + dy[1] + dz[2])
    double = rigidity + rigidity
    return (
        trace + double * dx[0],
        trace + double * dy[1],
        trace + double * dz[2],
        rigidity * (dy[0] + dx[1]),
        rigidity * (dz[0] + dx[2]),
        rigidity * (dz[1] + dy[2]),
    )


def force_of(stress, above, outward):
    nx, ny, nz, xy, xz, yz = stress
    up = [xz, yz, nz]
    if above is not None:
        up = [f - a for f, a in zip(up, (above[4], above[5], above[2]))]
    if outward is not None:
        up = [f * outward for f in up]
    return (
        behind(nx, 0) + behind(xy, 1) + up[0],
        behind(xy, 0) + behind(ny, 1) + up[1],
        behind(xz, 0) + behind(yz, 1) + up[2],
    )


def bf16_parts(value):
    parts = []
    for _ in range(3):
        part = value.astype(jnp.bfloat16)
        parts.append(part)
        value = value - part.astype(jnp.float32)
    return parts


def select_lanes(planes, matrix):
    rows = planes[0].shape[0]
    parts = bf16_parts(jnp.concatenate(planes, axis=0))
    product = jnp.dot(
        jnp.concatenate(parts, axis=0), matrix, preferred_element_type=jnp.float32
    )
    size = rows * len(planes)
    total = product[:size] + product[size : 2 * size] + product[2 * size :]
    return [total[k * rows : (k + 1) * rows] for k in range(len(planes))]


def select_rows(matrix, planes):
    lanes = planes[0].shape[1]
    parts = bf16_parts(jnp.concatenate(planes, axis=1))
    product = jnp.dot(
        jnp.concatenate([matrix] * 3, axis=1),
        jnp.concatenate(parts, axis=0),
        preferred_element_type=jnp.float32,
    )
    return [product[:, k * lanes : (k + 1) * lanes] for k in range(len(planes))]


def bf16_mask(condition):
    return jnp.where(condition, 1.0, 0.0).astype(jnp.bfloat16)


class Grids:
    def __init__(self, height, cheight, lanes, clanes, lane_of):
        def pairs(shape, fine_axis, size_of):
            f = lax.broadcasted_iota(jnp.int32, shape, fine_axis)
            c = lax.broadcasted_iota(jnp.int32, shape, 1 - fine_axis)
            return bf16_mask(size_of(f) == c)

        def row_of(f):
            turn = height - MARGIN // 2
            return jnp.right_shift(jnp.where(f < turn, f, f - height + 2 * cheight), 1)

        self.up_rows = pairs((height, cheight), 0, row_of)
        self.down_rows = pairs((cheight, height), 1, row_of)
        self.up_lanes = pairs((clanes, lanes), 1, lane_of)
        self.down_lanes = pairs((lanes, clanes), 0, lane_of)

    def prolong(self, planes):
        return select_rows(self.up_rows, select_lanes(planes, self.up_lanes))

    def restrict(self, planes):
        planes = select_lanes(select_rows(self.down_rows, planes), self.down_lanes)
        return [0.25 * plane for plane in planes]


def row_index(height, shape):
    index = lax.broadcasted_iota(jnp.int32, shape, 0)
    return jnp.where(index < height - MARGIN // 2, index, index - height)


def two_steps(dev, layers, clayers, fine, coarse, grids, keep_f, keep_c, state_f, state_c, out_f, out_c):
    depth, cdepth = 2 * layers, 2 * clayers
    scale = jnp.float32(time_step * time_step)
    three = range(3)
    ghost_f = grids.prolong([coarse(k, 0) for k in three])
    ghost_c = grids.restrict([fine(k, depth - 1) for k in three])

    def solver(plane, medium, ghost_above, ghost_below, last, stretched, first_layer):
        known = {}

        def here(g):
            if g < 0:
                return ghost_above
            if g == last + 1:
                return ghost_below
            return [plane(k, g) for k in three]

        def stress(g):
            if g < first_layer:
                return None
            if g not in known:
                top = max(g, 0)
                known[g] = stress_of(
                    here(g), here(g + 1), [medium(k, top) for k in (MU, LAM, W)[: 3 if stretched else 2]], stretched
                )
            return known[g]

        return stress

    zero_c = [jnp.zeros_like(ghost_c[0])] * 3
    stress_f = solver(fine, fine, None, ghost_f, depth - 1, True, 0)
    stress_c = solver(coarse, coarse, ghost_c, zero_c, cdepth - 1, False, -1)
    own = range(dev * layers, (dev + 1) * layers)
    cown = range(dev * clayers, (dev + 1) * clayers)
    near = sorted({max(own[0] - 1, 0), *own, min(own[-1] + 1, depth - 1)} | ({depth - 1} if dev == 0 else set()))
    cnear = sorted({0, max(cown[0] - 1, 0), *cown, min(cown[-1] + 1, cdepth - 1)})
    for g in near:
        force = force_of(stress_f(g), stress_f(g - 1), fine(W, g))
        rate = scale / fine(RHO, g)
        for k in three:
            u = fine(k, g)
            state_f[k, g] = jnp.where(keep_f(g), u + u - fine(Q + k, g) + force[k] * rate, 0.0)
    for g in cnear:
        force = force_of(stress_c(g), stress_c(g - 1), None)
        rate = (0.25 * scale) / coarse(RHO, g)
        for k in three:
            v = coarse(k, g)
            state_c[k, g] = jnp.where(keep_c, v + v - coarse(Q + k, g) + force[k] * rate, 0.0)

    ghost_f = ghost_c = None
    if dev == 1:
        ghost_f = grids.prolong([state_c[k, 0] for k in three])
    else:
        ghost_c = grids.restrict([state_f[k, depth - 1] for k in three])
    stress_f = solver(lambda k, g: state_f[k, g], fine, None, ghost_f, depth - 1, True, 0)
    stress_c = solver(lambda k, g: state_c[k, g], coarse, ghost_c, zero_c, cdepth - 1, False, -1)
    for l, g in enumerate(own):
        force = force_of(stress_f(g), stress_f(g - 1), fine(W, g))
        rate = scale / fine(RHO, g)
        for k in three:
            u = state_f[k, g]
            out_f(k, l, u + u - fine(k, g) + force[k] * rate)
    for l, g in enumerate(cown):
        force = force_of(stress_c(g), stress_c(g - 1), None)
        rate = (0.25 * scale) / coarse(RHO, g)
        for k in three:
            v = state_c[k, g]
            out_c(k, l, v + v - coarse(k, g) + force[k] * rate)


def for_each_core(body):
    dev = lax.axis_index("dev")

    @pl.when(dev == 0)
    def _():
        body(0)

    @pl.when(dev != 0)
    def _():
        body(1)


def inside(index, axis, size):
    at = index + lax.axis_index(axis) * size
    return (at >= 0) & (at < lax.axis_size(axis) * size)


def reader(dev, own, far, own_halo, far_halo):
    count = own.shape[1]

    def read(field, g, lanes=slice(None)):
        ref, edge = (own, own_halo) if g // count == dev else (far, far_halo)
        return jnp.concatenate(
            [ref[field, g % count, :, lanes], edge[field, g % count, :, lanes]], axis=0
        )

    return read


def ends_kernel(own_f, own_c, far_f, far_c, own_fh, own_ch, far_fh, far_ch, strip_f, strip_c):
    def body(dev):
        for own, far, own_halo, far_halo, strip, fields, room in (
            (own_f, far_f, own_fh, far_fh, strip_f, FINE_FIELDS, 4),
            (own_c, far_c, own_ch, far_ch, strip_c, COARSE_FIELDS, 2),
        ):
            read = reader(dev, own, far, own_halo, far_halo)
            wide = own.shape[3]
            lane = lax.broadcasted_iota(jnp.int32, strip.shape[2:], 1)
            for field in range(fields):
                for g in strip_layers(dev, own.shape[1], room == 4):
                    left = pltpu.roll(read(field, g, slice(0, LANES)), room, 1)
                    right = pltpu.roll(
                        read(field, g, slice(wide - LANES, wide)), LANES - room, 1
                    )
                    strip[field, g] = jnp.where(lane < LANES // 2, left, right)

    for_each_core(body)


def main_kernel(
    own_f, own_c, far_f, far_c, own_fh, own_ch, far_fh, far_ch, out_f, out_c, state_f, state_c
):
    layers, n, width = own_f.shape[1:]
    clayers, nc, cwidth = own_c.shape[1:]
    height, cheight = n + MARGIN, nc + MARGIN
    fx = row_index(height, (height, width))
    cx = row_index(cheight, (cheight, cwidth))
    rows_f = inside(fx, "gx", n) & (fx >= -1)
    keep_c = inside(cx, "gx", nc) & (cx >= -1) & (cx <= nc)
    grids = Grids(height, cheight, width, cwidth, lambda f: jnp.right_shift(f, 1))

    def body(dev):
        fine = reader(dev, own_f, far_f, own_fh, far_fh)
        coarse = reader(dev, own_c, far_c, own_ch, far_ch)

        def store_f(k, l, value):
            out_f[k, l] = value[:n]

        def store_c(k, l, value):
            out_c[k, l] = value[:nc]

        two_steps(
            dev, layers, clayers, fine, coarse, grids,
            lambda g: rows_f & (fx <= n + (g == 2 * layers - 1)), keep_c,
            state_f, state_c, store_f, store_c,
        )

    for_each_core(body)


def strip_layers(dev, count, fine):
    depth = 2 * count
    if fine:
        return range(depth) if dev == 0 else range(count - 2, depth)
    if dev == 0:
        return range(count + 2)
    return [0, 1, *range(count - 2, depth)]


def strip_kernel(
    strip_f, strip_c, main_f, main_c, own_ye, own_yo, far_ye, far_yo, out_f, out_c, fs, cs, state_f, state_c
):
    layers, n, width = main_f.shape[1:]
    clayers, nc, cwidth = main_c.shape[1:]
    height, cheight = n + MARGIN, nc + MARGIN
    fine_table, coarse_table = tables(layers, clayers)
    middle = LANES // 2
    fx = row_index(height, (height, LANES))
    cx = row_index(cheight, (cheight, LANES))
    lane_f = lax.broadcasted_iota(jnp.int32, (height, LANES), 1)
    lane_c = lax.broadcasted_iota(jnp.int32, (cheight, LANES), 1)
    fy = jnp.where(lane_f < middle, lane_f - 4, lane_f - LANES + 4 + width)
    cy = jnp.where(lane_c < middle, lane_c - 2, lane_c - LANES + 2 + cwidth)
    base_f = inside(fx, "gx", n) & inside(fy, "gy", width) & (fx >= -1) & (fy >= -1)
    keep_c = (
        inside(cx, "gx", nc) & inside(cy, "gy", cwidth)
        & (cx >= -1) & (cx <= nc) & (cy >= -1) & (cy <= cwidth)
    )
    grids = Grids(
        height, cheight, LANES, LANES,
        lambda f: jnp.right_shift(f, 1) + jnp.where(f < middle, 0, middle),
    )
    even = lax.rem(lax.axis_index("gy"), 2) == 0

    def body(dev):
        for table, src, dst, top, count, room, lane in (
            (fine_table, strip_f, fs, 0, layers, 4, lane_f),
            (coarse_table, strip_c, cs, height, clayers, 2, lane_c),
        ):
            rows = src.shape[2]
            for near in (True, False):
                e, o = (own_ye, own_yo) if near else (far_ye, far_yo)
                e, o = e[top : top + rows, :], o[top : top + rows, :]
                highs, lows = jnp.where(even, e, o), jnp.where(even, o, e)
                for field, layer, high, low, offset in table:
                    g = (dev if near else 1 - dev) * count + layer
                    if g not in strip_layers(dev, count, room == 4):
                        continue
                    start = LANES - room
                    value = src[field, g]
                    value = jnp.where(
                        (lane >= start) & (lane < start + high),
                        pltpu.roll(highs, (start - offset) % LANES, 1), value,
                    )
                    start = room - low
                    value = jnp.where(
                        (lane >= start) & (lane < start + low),
                        pltpu.roll(lows, (start - offset) % LANES, 1), value,
                    )
                    dst[field, g] = value

        def put(out, main, k, l, value, cells, room):
            wide = out.shape[3]
            lane = lax.broadcasted_iota(jnp.int32, (cells, LANES), 1)
            first = pltpu.roll(value[:cells], LANES - room, 1)
            last = pltpu.roll(value[:cells], room, 1)
            for start in range(0, wide, LANES):
                part = main[k, l, :, start : start + LANES]
                if start == 0:
                    part = jnp.where(lane < room, first, part)
                if start == wide - LANES:
                    part = jnp.where(lane >= LANES - room, last, part)
                out[k, l, :, start : start + LANES] = part

        two_steps(
            dev, layers, clayers,
            lambda field, g: fs[field, g], lambda field, g: cs[field, g], grids,
            lambda g: base_f & (fx <= n + (g == 2 * layers - 1)) & (fy <= width + (g == 2 * layers - 1)),
            keep_c, state_f, state_c,
            lambda k, l, value: put(out_f, main_f, k, l, value, n, 4),
            lambda k, l, value: put(out_c, main_c, k, l, value, nc, 2),
        )

    for_each_core(body)


def partners(count, parity):
    pairs = [(i, ((i + parity) ^ 1) - parity) for i in range(count)]
    return [(i, j) for i, j in pairs if 0 <= j < count]


def swap(value, axis, parity):
    return lax.ppermute(value, axis, partners(lax.axis_size(axis), parity))


def call(kernel, out_shape, operands, scratch=(), flops=0, space=pltpu.VMEM, limit=24):
    size = sum(o.size for o in out_shape) * 4
    call = pl.pallas_call(
        kernel,
        out_shape=out_shape,
        in_specs=[pl.BlockSpec(memory_space=space)] * len(operands),
        out_specs=[pl.BlockSpec(memory_space=pltpu.VMEM)] * len(out_shape),
        scratch_shapes=list(scratch),
        cost_estimate=pl.CostEstimate(flops=flops, bytes_accessed=size, transcendentals=0),
        compiler_params=pltpu.CompilerParams(vmem_limit_bytes=limit * 1024 * 1024),
    )
    if space == pltpu.HBM:
        operands = [pltpu.with_memory_space_constraint(o, space) for o in operands]
    return call(*operands)


def shape(*dims):
    return jax.ShapeDtypeStruct(dims, jnp.float32)


def per_device(*inputs):
    _, layers, n, width = inputs[0].shape
    _, clayers, nc, cwidth = inputs[3].shape
    grids = grid_tables(inputs[0].shape, inputs[3].shape)
    rows = max(edge_rows(*grids, first)[1] for first in (True, False))
    height, cheight = n + MARGIN, nc + MARGIN

    edge = shape(rows, LANES)
    own_f, own_c, to_even, to_odd = call(
        pack_x_kernel,
        (shape(FINE_FIELDS, layers, n, width), shape(COARSE_FIELDS, clayers, nc, cwidth), edge, edge),
        inputs,
        scratch=(pltpu.SemaphoreType.DMA((6,)),),
        space=pltpu.HBM,
        limit=24,
    )
    got_odd = swap(to_odd, "gx", 1)
    got_even = swap(to_even, "gx", 0)
    far_f, far_c = swap(own_f, "dev", 0), swap(own_c, "dev", 0)

    inner = shape(n + nc, LANES)
    firsts, lasts = call(pack_inner_kernel, (inner, inner), (own_f, own_c))

    side = shape(height + cheight, LANES)
    own_fh, own_ch, to_even, to_odd = call(
        functools.partial(pack_y_kernel, n),
        (
            shape(FINE_FIELDS, layers, MARGIN, width),
            shape(COARSE_FIELDS, clayers, MARGIN, cwidth),
            side,
            side,
        ),
        (firsts, lasts, got_even, got_odd),
    )
    own_yo = swap(to_odd, "gy", 1)
    own_ye = swap(to_even, "gy", 0)
    far_fh, far_ch = swap(own_fh, "dev", 0), swap(own_ch, "dev", 0)

    def states(lanes, clanes):
        return (
            pltpu.VMEM((3, 2 * layers, height, lanes), jnp.float32),
            pltpu.VMEM((3, 2 * clayers, cheight, clanes), jnp.float32),
        )

    results = (shape(*inputs[0].shape), shape(*inputs[3].shape))
    strips = (
        (FINE_FIELDS, 2 * layers, height, LANES),
        (COARSE_FIELDS, 2 * clayers, cheight, LANES),
    )
    tiles = (own_f, own_c, far_f, far_c, own_fh, own_ch, far_fh, far_ch)
    main_f, main_c = call(
        main_kernel, results, tiles, scratch=states(width, cwidth), flops=MAIN_FLOPS
    )
    strip_f, strip_c = call(ends_kernel, tuple(shape(*dims) for dims in strips), tiles)
    far_yo, far_ye = swap(own_yo, "dev", 0), swap(own_ye, "dev", 0)
    return call(
        strip_kernel,
        results,
        (strip_f, strip_c, main_f, main_c, own_ye, own_yo, far_ye, far_yo),
        scratch=tuple(pltpu.VMEM(dims, jnp.float32) for dims in strips) + states(LANES, LANES),
    )


MAIN_FLOPS = 4_000_000


def solution(mesh):
    spec = P(None, "dev", "gx", "gy")

    return jax.shard_map(
        per_device,
        mesh=mesh,
        in_specs=(spec,) * 6,
        out_specs=(spec, spec),
        check_vma=False,
    )
```

```python
import functools

import jax
import jax.numpy as jnp
from jax import lax
from jax.experimental import pallas as pl
from jax.experimental.pallas import tpu as pltpu
from jax.sharding import PartitionSpec as P


time_step = 0.15
LANES = 128
MARGIN = 8
U, Q, RHO, MU, LAM, W = 0, 3, 6, 7, 8, 9
FINE_FIELDS, COARSE_FIELDS = 10, 9


def fine_widths(field, layer, layers):
    bottom, above = layer == layers - 1, layer == layers - 2
    if field < Q:
        return (4 if bottom else 3 if above else 2), 2
    if field <= RHO:
        return (2 if bottom else 1), 1
    return (2 if bottom or above else 1), 2


def coarse_widths(field):
    if field < Q:
        return 2, 2
    if field <= RHO:
        return 1, 1
    return 1, 2


def plane_table(fields, layers, widths, slot, span):
    assert 2 * layers * span == LANES
    table = []
    for layer in range(layers):
        for field in range(fields):
            high, low = widths(field, layer)
            table.append((field, layer, high, low, slot(field) + layer * span))
    return table


def fine_slot(field):
    if field < Q:
        return 4 * field
    if field in (MU, LAM):
        return 12 + 2 * (field - MU)
    return LANES // 2 + {W: 0, Q: 2, Q + 1: 4, Q + 2: 6, RHO: 8}[field]


def coarse_slot(field):
    if field < Q:
        return 2 * field
    return 6 if field == MU else LANES // 2 + {LAM: 0, Q: 2, Q + 1: 3, Q + 2: 4, RHO: 5}[field]


def round_up(value, multiple):
    return -(-value // multiple) * multiple


FINE_SPAN, COARSE_SPAN = 16, 8


def tables(fine_layers, coarse_layers):
    fine = plane_table(
        FINE_FIELDS, fine_layers, lambda f, l: fine_widths(f, l, fine_layers), fine_slot, FINE_SPAN
    )
    coarse = plane_table(
        COARSE_FIELDS, coarse_layers, lambda f, l: coarse_widths(f), coarse_slot, COARSE_SPAN
    )
    return fine, coarse


def edge_rows(tables_of_grids, parts_of_grids, first):
    pieces, at = [], 0
    for grid, (table, parts) in enumerate(zip(tables_of_grids, parts_of_grids)):
        for field, layer, high, low, _ in table:
            size = high if first else low
            for t in range(parts):
                pieces.append((grid, field, layer, t, size, at))
                at += size
    return pieces, round_up(at, 8)


def grid_tables(fine_shape, coarse_shape):
    fine, coarse = tables(fine_shape[1], coarse_shape[1])
    return (fine, coarse), (fine_shape[3] // LANES, coarse_shape[3] // LANES)


def pack_x_kernel(fu, fp, fm, cu, cp, cm, fine, coarse, to_even, to_odd, sems):
    copies = []
    for out, sources in ((fine, (fu, fp, fm)), (coarse, (cu, cp, cm))):
        for first, source in zip((U, Q, RHO), sources):
            copies.append(
                pltpu.make_async_copy(
                    source, out.at[first : first + source.shape[0]], sems.at[len(copies)]
                )
            )
    for copy in copies:
        copy.start()
    for copy in copies:
        copy.wait()
    grids = grid_tables(fine.shape, coarse.shape)

    def fill(out, first):
        for grid, field, layer, t, size, at in edge_rows(*grids, first)[0]:
            ref = (fine, coarse)[grid]
            start = 0 if first else ref.shape[2] - size
            out[at : at + size, :] = ref[
                field, layer, start : start + size, t * LANES : (t + 1) * LANES
            ]

    even = lax.rem(lax.axis_index("gx"), 2) == 0

    @pl.when(even)
    def _():
        fill(to_even, False)
        fill(to_odd, True)

    @pl.when(jnp.logical_not(even))
    def _():
        fill(to_even, True)
        fill(to_odd, False)


class Bundle:
    def __init__(self, fine_shape, coarse_shape):
        self.layers = fine_shape[1], coarse_shape[1]
        self.parts = fine_shape[3] // LANES, coarse_shape[3] // LANES
        self.rows = fine_shape[2] // 8 + 1, coarse_shape[2] // 8 + 1
        self.halo_base, self.ends_base, at = [], [], 0
        for grid, fields in enumerate((FINE_FIELDS, COARSE_FIELDS)):
            self.halo_base.append(at)
            at += fields * self.layers[grid] * self.parts[grid]
            self.ends_base.append(at)
            at += fields * self.rows[grid]
        self.size = at

    def halo(self, grid, field, layer, part):
        return self.halo_base[grid] + (field * self.layers[grid] + layer) * self.parts[grid] + part

    def ends(self, ref, grid, field):
        base = self.ends_base[grid] + field * self.rows[grid]
        return jnp.concatenate([ref[base + r] for r in range(self.rows[grid])], axis=0)


def end_columns(read, layers, span):
    for layer in range(layers):
        first, last = read(layer)
        lane = lax.broadcasted_iota(jnp.int32, first.shape, 1)
        value = jnp.where(lane < LANES // 2, first, last)
        value = pltpu.roll(value, layer * span + span // 2, 1)
        total = value if layer == 0 else jnp.where(lane >= layer * span, value, total)
    return total


def pack_inner_kernel(fine, coarse, fine_ends, coarse_ends):
    for ref, out, span in ((fine, fine_ends, FINE_SPAN), (coarse, coarse_ends, COARSE_SPAN)):
        for field in range(ref.shape[0]):

            def read(layer):
                return ref[field, layer, :, :LANES], ref[field, layer, :, ref.shape[3] - LANES :]

            out[field] = end_columns(read, ref.shape[1], span)


def pack_y_kernel(bundle, fine_ends, coarse_ends, got_even, got_odd, out, to_even, to_odd):
    grids = tables(*bundle.layers), bundle.parts

    def halo(high_ref, low_ref):
        for first, ref in ((True, high_ref), (False, low_ref)):
            for grid, field, layer, t, size, at in edge_rows(*grids, first)[0]:
                start = 0 if first else MARGIN - size
                out[bundle.halo(grid, field, layer, t), start : start + size, :] = ref[
                    at : at + size, :
                ]

    for grid, table in enumerate(grids[0]):
        for field, layer, *_ in table:
            for t in range(bundle.parts[grid]):
                out[bundle.halo(grid, field, layer, t)] = jnp.zeros((MARGIN, LANES), jnp.float32)

    even = lax.rem(lax.axis_index("gx"), 2) == 0

    @pl.when(even)
    def _():
        halo(got_even, got_odd)

    @pl.when(jnp.logical_not(even))
    def _():
        halo(got_odd, got_even)

    packed = []
    for grid, (table, inner, span) in enumerate(
        zip(grids[0], (fine_ends, coarse_ends), (FINE_SPAN, COARSE_SPAN))
    ):
        rows = inner.shape[1] + MARGIN
        lane = lax.broadcasted_iota(jnp.int32, (rows, LANES), 1)
        within = jnp.bitwise_and(lane, span - 1)
        sides = [[None, None], [None, None]]
        for field, layer, high, low, slot in sorted(table, key=lambda entry: entry[4]):
            if layer:
                continue

            def read(layer):
                parts = (0, bundle.parts[grid] - 1)
                return [out[bundle.halo(grid, field, layer, t)] for t in parts]

            ends = jnp.concatenate(
                [inner[field], end_columns(read, bundle.layers[grid], span)], axis=0
            )
            base = bundle.ends_base[grid] + field * bundle.rows[grid]
            for r in range(bundle.rows[grid]):
                out[base + r] = ends[r * 8 : (r + 1) * 8]
            half, start = divmod(slot, LANES // 2)
            for side, first in enumerate((span // 2, span // 2 - low)):
                shift = (slot - first) % LANES
                value = pltpu.roll(ends, shift, 1) if shift else ends
                before = sides[side][half]
                sides[side][half] = (
                    value if before is None else jnp.where(within >= start, value, before)
                )
        packed.append([jnp.where(lane < LANES // 2, lower, upper) for lower, upper in sides])
    even_y = lax.rem(lax.axis_index("gy"), 2) == 0

    def place(first_out, last_out):
        at = 0
        for firsts, lasts in packed:
            rows = slice(at, at + firsts.shape[0])
            first_out[rows, :] = firsts
            last_out[rows, :] = lasts
            at += firsts.shape[0]

    @pl.when(even_y)
    def _():
        place(to_odd, to_even)

    @pl.when(jnp.logical_not(even_y))
    def _():
        place(to_even, to_odd)


def ahead(value, axis):
    return pltpu.roll(value, value.shape[axis] - 1, axis)


def behind(value, axis):
    return value - pltpu.roll(value, 1, axis)


def stress_of(here, below, medium, stretched):
    rigidity, lame = medium[0], medium[1]
    dx = [ahead(f, 0) - f for f in here]
    dy = [ahead(f, 1) - f for f in here]
    dz = [b - f for b, f in zip(below, here)]
    if stretched:
        dz = [f * medium[2] for f in dz]
    trace = lame * (dx[0] + dy[1] + dz[2])
    double = rigidity + rigidity
    return (
        trace + double * dx[0],
        trace + double * dy[1],
        trace + double * dz[2],
        rigidity * (dy[0] + dx[1]),
        rigidity * (dz[0] + dx[2]),
        rigidity * (dz[1] + dy[2]),
    )


def force_of(stress, above, outward):
    nx, ny, nz, xy, xz, yz = stress
    up = [xz, yz, nz]
    if above is not None:
        up = [f - a for f, a in zip(up, (above[4], above[5], above[2]))]
    if outward is not None:
        up = [f * outward for f in up]
    return (
        behind(nx, 0) + behind(xy, 1) + up[0],
        behind(xy, 0) + behind(ny, 1) + up[1],
        behind(xz, 0) + behind(yz, 1) + up[2],
    )


def bf16_parts(value):
    parts = []
    for _ in range(3):
        part = value.astype(jnp.bfloat16)
        parts.append(part)
        value = value - part.astype(jnp.float32)
    return parts


def select_lanes(planes, matrix):
    rows = planes[0].shape[0]
    parts = bf16_parts(jnp.concatenate(planes, axis=0))
    product = jnp.dot(
        jnp.concatenate(parts, axis=0), matrix, preferred_element_type=jnp.float32
    )
    size = rows * len(planes)
    total = product[:size] + product[size : 2 * size] + product[2 * size :]
    return [total[k * rows : (k + 1) * rows] for k in range(len(planes))]


def select_rows(matrix, planes):
    lanes = planes[0].shape[1]
    parts = bf16_parts(jnp.concatenate(planes, axis=1))
    product = jnp.dot(
        jnp.concatenate([matrix] * 3, axis=1),
        jnp.concatenate(parts, axis=0),
        preferred_element_type=jnp.float32,
    )
    return [product[:, k * lanes : (k + 1) * lanes] for k in range(len(planes))]


def bf16_mask(condition):
    return jnp.where(condition, 1.0, 0.0).astype(jnp.bfloat16)


class Grids:
    def __init__(self, height, cheight, lanes, clanes, lane_of):
        def pairs(shape, fine_axis, size_of):
            f = lax.broadcasted_iota(jnp.int32, shape, fine_axis)
            c = lax.broadcasted_iota(jnp.int32, shape, 1 - fine_axis)
            return bf16_mask(size_of(f) == c)

        def row_of(f):
            turn = height - MARGIN // 2
            return jnp.right_shift(jnp.where(f < turn, f, f - height + 2 * cheight), 1)

        self.up_rows = pairs((height, cheight), 0, row_of)
        self.down_rows = pairs((cheight, height), 1, row_of)
        self.up_lanes = pairs((clanes, lanes), 1, lane_of)
        self.down_lanes = pairs((lanes, clanes), 0, lane_of)

    def prolong(self, planes):
        return select_rows(self.up_rows, select_lanes(planes, self.up_lanes))

    def restrict(self, planes):
        planes = select_lanes(select_rows(self.down_rows, planes), self.down_lanes)
        return [0.25 * plane for plane in planes]


def row_index(height, shape):
    index = lax.broadcasted_iota(jnp.int32, shape, 0)
    return jnp.where(index < height - MARGIN // 2, index, index - height)


def solver(plane, medium, ghost_above, ghost_below, last, stretched):
    known = {}

    def here(g):
        if g < 0:
            return ghost_above
        if g == last + 1:
            return ghost_below
        return [plane(k, g) for k in range(3)]

    def stress(g):
        if g < 0 and ghost_above is None:
            return None
        if g not in known:
            fields = (MU, LAM, W) if stretched else (MU, LAM)
            known[g] = stress_of(
                here(g), here(g + 1), [medium(k, max(g, 0)) for k in fields], stretched
            )
        return known[g]

    return stress


def advance(plane, before, medium, stress, g, scale, stretched):
    force = force_of(stress(g), stress(g - 1), medium(W, g) if stretched else None)
    rate = scale / medium(RHO, g)
    return [
        plane(k, g) + plane(k, g) - before(k, g) + force[k] * rate for k in range(3)
    ]


def step_scales():
    scale = jnp.float32(time_step * time_step)
    return scale, 0.25 * scale


def first_step(dev, layers, clayers, fine, coarse, grids, keep_f, keep_c, state_f, state_c):
    depth, cdepth = 2 * layers, 2 * clayers
    scale, cscale = step_scales()
    three = range(3)
    ghost_f = grids.prolong([coarse(k, 0) for k in three])
    ghost_c = grids.restrict([fine(k, depth - 1) for k in three])
    zero_c = [jnp.zeros_like(ghost_c[0])] * 3
    stress_f = solver(fine, fine, None, ghost_f, depth - 1, True)
    stress_c = solver(coarse, coarse, ghost_c, zero_c, cdepth - 1, False)
    near = {*range(max(dev * layers - 1, 0), min((dev + 1) * layers + 1, depth)), depth - 1}
    cnear = {0, *range(max(dev * clayers - 1, 0), min((dev + 1) * clayers + 1, cdepth))}
    for g in sorted(near):
        values = advance(fine, lambda k, g: fine(Q + k, g), fine, stress_f, g, scale, True)
        for k in three:
            state_f[k, g] = jnp.where(keep_f(g), values[k], 0.0)
    for g in sorted(cnear):
        values = advance(coarse, lambda k, g: coarse(Q + k, g), coarse, stress_c, g, cscale, False)
        for k in three:
            state_c[k, g] = jnp.where(keep_c, values[k], 0.0)


def second_step(dev, layers, clayers, fine, coarse, grids, state_f, state_c, out_f, out_c):
    depth, cdepth = 2 * layers, 2 * clayers
    scale, cscale = step_scales()
    ghost_f = ghost_c = None
    if dev == 1:
        ghost_f = grids.prolong([state_c[k, 0] for k in range(3)])
    else:
        ghost_c = grids.restrict([state_f[k, depth - 1] for k in range(3)])
    zero_c = [jnp.zeros(state_c.shape[2:], jnp.float32)] * 3
    now_f, now_c = lambda k, g: state_f[k, g], lambda k, g: state_c[k, g]
    stress_f = solver(now_f, fine, None, ghost_f, depth - 1, True)
    stress_c = solver(now_c, coarse, ghost_c, zero_c, cdepth - 1, False)
    for l in range(layers):
        values = advance(now_f, fine, fine, stress_f, dev * layers + l, scale, True)
        for k in range(3):
            out_f[k, l] = values[k][: out_f.shape[2]]
    for l in range(clayers):
        values = advance(now_c, coarse, coarse, stress_c, dev * clayers + l, cscale, False)
        for k in range(3):
            out_c[k, l] = values[k][: out_c.shape[2]]


def for_each_core(body):
    dev = lax.axis_index("dev")

    @pl.when(dev == 0)
    def _():
        body(0)

    @pl.when(dev != 0)
    def _():
        body(1)


def inside(index, axis, size):
    at = index + lax.axis_index(axis) * size
    return (at >= 0) & (at < lax.axis_size(axis) * size)


def readers(dev, bundle, own_f, own_c, far_f, far_c, own_b, far_b):
    def reader(grid, own, far):
        def read(field, g):
            layer = g % bundle.layers[grid]
            mine = g // bundle.layers[grid] == dev
            ref, tiles = (own, own_b) if mine else (far, far_b)
            halo = [
                tiles[bundle.halo(grid, field, layer, t)] for t in range(bundle.parts[grid])
            ]
            return jnp.concatenate([ref[field, layer], jnp.concatenate(halo, axis=1)], axis=0)

        return read

    return reader(0, own_f, far_f), reader(1, own_c, far_c)


def tile_grids(own_f, own_c):
    return Grids(
        own_f.shape[2] + MARGIN, own_c.shape[2] + MARGIN, own_f.shape[3], own_c.shape[3],
        lambda f: jnp.right_shift(f, 1),
    )


def first_kernel(bundle, own_f, own_c, far_f, far_c, own_b, far_b, state_f, state_c):
    _, layers, n, width = own_f.shape
    _, clayers, nc, cwidth = own_c.shape
    fx = row_index(n + MARGIN, (n + MARGIN, width))
    cx = row_index(nc + MARGIN, (nc + MARGIN, cwidth))
    rows_f = inside(fx, "gx", n) & (fx >= -1)
    keep_c = inside(cx, "gx", nc) & (cx >= -1) & (cx <= nc)
    grids = tile_grids(own_f, own_c)

    def body(dev):
        fine, coarse = readers(dev, bundle, own_f, own_c, far_f, far_c, own_b, far_b)
        first_step(
            dev, layers, clayers, fine, coarse, grids,
            lambda g: rows_f & (fx <= n + (g == 2 * layers - 1)), keep_c, state_f, state_c,
        )

    for_each_core(body)


def second_kernel(
    bundle, own_f, own_c, far_f, far_c, own_b, far_b, state_f, state_c, out_f, out_c, strip_f, strip_c
):
    grids = tile_grids(own_f, own_c)

    def body(dev):
        fine, coarse = readers(dev, bundle, own_f, own_c, far_f, far_c, own_b, far_b)
        second_step(
            dev, own_f.shape[1], own_c.shape[1], fine, coarse, grids, state_f, state_c, out_f, out_c
        )

    for_each_core(body)
    top = lax.axis_index("dev") == 0
    for grid, (strip, span) in enumerate(((strip_f, FINE_SPAN), (strip_c, COARSE_SPAN))):
        lane = lax.broadcasted_iota(jnp.int32, (strip.shape[1], LANES), 1)
        for field in range(strip.shape[0]):
            own, far = bundle.ends(own_b, grid, field), bundle.ends(far_b, grid, field)
            upper, lower = jnp.where(top, own, far), jnp.where(top, far, own)
            whole = jnp.where(lane < LANES // 2, upper, pltpu.roll(lower, LANES // 2, 1))
            strip[field, :, :LANES] = pltpu.roll(whole, LANES - span // 4, 1)
            strip[field, :, LANES:] = whole


def strip_kernel(
    strip_f, strip_c, main_f, main_c, own_ye, own_yo, far_ye, far_yo, out_f, out_c
):
    layers, n, width = main_f.shape[1:]
    clayers, nc, cwidth = main_c.shape[1:]
    height, cheight = n + MARGIN, nc + MARGIN
    depth, cdepth = 2 * layers, 2 * clayers
    fine_table, coarse_table = tables(layers, clayers)
    three = range(3)
    top = lax.axis_index("dev") == 0
    even = lax.rem(lax.axis_index("gy"), 2) == 0
    wide = 2 * LANES

    def places(rows, span, extent):
        lane = lax.broadcasted_iota(jnp.int32, (rows, wide), 1)
        low = lane < LANES
        inner = jnp.bitwise_and(lane, LANES - 1)
        within = jnp.bitwise_and(lane, span - 1)
        room = span // 4
        at = jnp.where(low, within - room, within + extent - span // 2)
        used = within < span - room
        return jnp.right_shift(inner, span.bit_length() - 1), at, used

    fg, fy, used_f = places(height, FINE_SPAN, width)
    cg, cy, used_c = places(cheight, COARSE_SPAN, cwidth)
    fx, cx = row_index(height, (height, wide)), row_index(cheight, (cheight, wide))
    last = (fg == depth - 1).astype(jnp.int32)
    keep_f = (
        used_f & inside(fx, "gx", n) & inside(fy, "gy", width)
        & (fx >= -1) & (fy >= -1) & (fx <= n + last) & (fy <= width + last)
    )
    keep_c = (
        used_c & inside(cx, "gx", nc) & inside(cy, "gy", cwidth)
        & (cx >= -1) & (cx <= nc) & (cy >= -1) & (cy <= cwidth)
    )

    def filled(table, src, start, span):
        rows = src.shape[1]
        room = span // 4
        lane = lax.broadcasted_iota(jnp.int32, (rows, LANES), 1)
        within = jnp.bitwise_and(lane, span - 1)
        sides = []
        for e, o in ((own_ye, own_yo), (far_ye, far_yo)):
            e, o = e[start : start + rows, :], o[start : start + rows, :]
            sides.append((jnp.where(even, o, e), jnp.where(even, e, o)))
        uppers = [jnp.where(top, a, b) for a, b in zip(*sides)]
        lowers = [jnp.where(top, b, a) for a, b in zip(*sides)]
        fields = []
        for field in range(src.shape[0]):
            entries = [entry for entry in table if entry[0] == field]
            slot = entries[0][4]
            width_of = (max(e[3] for e in entries), max(e[2] for e in entries))
            parts = []
            for side in range(2):
                size = width_of[side]
                first = span // 2 if side else room - size
                shift = (first - slot) % LANES
                halo = jnp.where(
                    lane < LANES // 2,
                    pltpu.roll(uppers[side], shift, 1) if shift else uppers[side],
                    pltpu.roll(lowers[side], (shift + LANES // 2) % LANES, 1),
                )
                parts.append(
                    jnp.where(
                        (within >= first) & (within < first + size),
                        halo,
                        src[field, :, side * LANES : (side + 1) * LANES],
                    )
                )
            fields.append(jnp.concatenate(parts, axis=1))
        return fields

    fine = filled(fine_table, strip_f, 0, FINE_SPAN)
    coarse = filled(coarse_table, strip_c, height, COARSE_SPAN)

    def fine_lane(f):
        tile, inner = jnp.bitwise_and(f, LANES), jnp.bitwise_and(f, LANES - 1)
        bottom = inner - (depth - 1) * FINE_SPAN
        return jnp.where(bottom >= 0, tile + jnp.right_shift(bottom, 1), -1)

    grids = Grids(height, cheight, wide, wide, fine_lane)
    scale = jnp.float32(time_step * time_step)

    def shifted(value, lanes):
        return pltpu.roll(value, lanes % wide, 1)

    def lift(stress, lanes, at_top, above):
        return [jnp.where(at_top, a, shifted(stress[k], lanes)) for k, a in zip((2, 4, 5), above)]

    def step(u, p, v, q):
        ghost_f = grids.prolong(v)
        ghost_c = grids.restrict(u)
        below = [jnp.where(fg == depth - 1, b, shifted(f, -FINE_SPAN)) for f, b in zip(u, ghost_f)]
        stress = stress_of(u, below, [fine[k] for k in (MU, LAM, W)], True)
        up = lift(stress, FINE_SPAN, fg == 0, [0.0] * 3)
        force = force_of(stress, {2: up[0], 4: up[1], 5: up[2]}, fine[W])
        rate = scale / fine[RHO]
        next_u = [a + a - b + f * rate for a, b, f in zip(u, p, force)]
        medium = [coarse[k] for k in (MU, LAM)]
        under = [jnp.where(cg == cdepth - 1, 0.0, shifted(f, -COARSE_SPAN)) for f in v]
        stress = stress_of(v, under, medium, False)
        above = stress_of(ghost_c, v, medium, False)
        up = lift(stress, COARSE_SPAN, cg == 0, [above[k] for k in (2, 4, 5)])
        force = force_of(stress, {2: up[0], 4: up[1], 5: up[2]}, None)
        rate = (0.25 * scale) / coarse[RHO]
        next_v = [a + a - b + f * rate for a, b, f in zip(v, q, force)]
        return next_u, next_v

    u, v = fine[:3], coarse[:3]
    next_u, next_v = step(u, fine[Q:RHO], v, coarse[Q:RHO])
    next_u = [jnp.where(keep_f, f, 0.0) for f in next_u]
    next_v = [jnp.where(keep_c, f, 0.0) for f in next_v]
    last_u, last_v = step(next_u, u, next_v, v)

    for values, out, main, span in (
        (last_u, out_f, main_f, FINE_SPAN),
        (last_v, out_c, main_c, COARSE_SPAN),
    ):
        cells, extent = out.shape[2:]
        room = span // 4
        lane = lax.broadcasted_iota(jnp.int32, (cells, LANES), 1)
        for k in three:
            ends = [values[k][:cells, side * LANES : (side + 1) * LANES] for side in range(2)]
            ends = [jnp.where(top, e, pltpu.roll(e, LANES // 2, 1)) for e in ends]
            for l in range(out.shape[1]):
                first = pltpu.roll(ends[0], LANES - l * span - room, 1)
                final = pltpu.roll(ends[1], LANES - l * span - span // 2, 1)
                for start in range(0, extent, LANES):
                    part = main[k, l, :, start : start + LANES]
                    if start == 0:
                        part = jnp.where(lane < room, first, part)
                    if start == extent - LANES:
                        part = jnp.where(lane >= LANES - room, final, part)
                    out[k, l, :, start : start + LANES] = part


def partners(count, parity):
    pairs = [(i, ((i + parity) ^ 1) - parity) for i in range(count)]
    return [(i, j) for i, j in pairs if 0 <= j < count]


def swap(value, axis, parity):
    return lax.ppermute(value, axis, partners(lax.axis_size(axis), parity))


def call(kernel, out_shape, operands, scratch=(), flops=0, space=pltpu.VMEM, limit=24):
    size = sum(o.size for o in out_shape) * 4
    call = pl.pallas_call(
        kernel,
        out_shape=out_shape,
        in_specs=[pl.BlockSpec(memory_space=space)] * len(operands),
        out_specs=[pl.BlockSpec(memory_space=pltpu.VMEM)] * len(out_shape),
        scratch_shapes=list(scratch),
        cost_estimate=pl.CostEstimate(flops=flops, bytes_accessed=size, transcendentals=0),
        compiler_params=pltpu.CompilerParams(vmem_limit_bytes=limit * 1024 * 1024),
    )
    if space == pltpu.HBM:
        operands = [pltpu.with_memory_space_constraint(o, space) for o in operands]
    return call(*operands)


def shape(*dims):
    return jax.ShapeDtypeStruct(dims, jnp.float32)


def per_device(*inputs):
    _, layers, n, width = inputs[0].shape
    _, clayers, nc, cwidth = inputs[3].shape
    grids = grid_tables(inputs[0].shape, inputs[3].shape)
    rows = max(edge_rows(*grids, first)[1] for first in (True, False))
    height, cheight = n + MARGIN, nc + MARGIN

    edge = shape(rows, LANES)
    own_f, own_c, to_even, to_odd = call(
        pack_x_kernel,
        (shape(FINE_FIELDS, layers, n, width), shape(COARSE_FIELDS, clayers, nc, cwidth), edge, edge),
        inputs,
        scratch=(pltpu.SemaphoreType.DMA((6,)),),
        space=pltpu.HBM,
        limit=24,
    )
    got_odd = swap(to_odd, "gx", 1)
    got_even = swap(to_even, "gx", 0)
    far_f, far_c = swap(own_f, "dev", 0), swap(own_c, "dev", 0)

    fine_ends, coarse_ends = call(
        pack_inner_kernel,
        (shape(FINE_FIELDS, n, LANES), shape(COARSE_FIELDS, nc, LANES)),
        (own_f, own_c),
    )

    bundle = Bundle(inputs[0].shape, inputs[3].shape)
    side = shape(height + cheight, LANES)
    own_b, to_even, to_odd = call(
        functools.partial(pack_y_kernel, bundle),
        (shape(bundle.size, 8, LANES), side, side),
        (fine_ends, coarse_ends, got_even, got_odd),
    )
    own_yo = swap(to_odd, "gy", 1)
    own_ye = swap(to_even, "gy", 0)
    far_b = swap(own_b, "dev", 0)

    tiles = (own_f, own_c, far_f, far_c, own_b, far_b)
    states = call(
        functools.partial(first_kernel, bundle),
        (shape(3, 2 * layers, height, width), shape(3, 2 * clayers, cheight, cwidth)),
        tiles,
        flops=STEP_FLOPS,
    )
    results = (shape(*inputs[0].shape), shape(*inputs[3].shape))
    strips = (
        shape(FINE_FIELDS, height, 2 * LANES),
        shape(COARSE_FIELDS, cheight, 2 * LANES),
    )
    main_f, main_c, strip_f, strip_c = call(
        functools.partial(second_kernel, bundle),
        results + strips,
        tiles + tuple(states),
        flops=STEP_FLOPS,
    )
    far_yo, far_ye = swap(own_yo, "dev", 0), swap(own_ye, "dev", 0)
    return call(
        strip_kernel, results, (strip_f, strip_c, main_f, main_c, own_ye, own_yo, far_ye, far_yo)
    )


STEP_FLOPS = 2_000_000


def solution(mesh):
    spec = P(None, "dev", "gx", "gy")

    return jax.shard_map(
        per_device,
        mesh=mesh,
        in_specs=(spec,) * 6,
        out_specs=(spec, spec),
        check_vma=False,
    )
```

```python
import functools

import jax
import jax.numpy as jnp
from jax import lax
from jax.experimental import pallas as pl
from jax.experimental.pallas import tpu as pltpu
from jax.sharding import PartitionSpec as P


time_step = 0.15
LANES = 128
MARGIN = 8
U, Q, RHO, MU, LAM, W = 0, 3, 6, 7, 8, 9
FINE_FIELDS, COARSE_FIELDS = 10, 9


def fine_widths(field, layer, layers):
    bottom, above = layer == layers - 1, layer == layers - 2
    if field < Q:
        return (4 if bottom else 3 if above else 2), 2
    if field <= RHO:
        return (2 if bottom else 1), 1
    return (2 if bottom or above else 1), 2


def coarse_widths(field):
    if field < Q:
        return 2, 2
    if field <= RHO:
        return 1, 1
    return 1, 2


def plane_table(fields, layers, widths, slot, span):
    assert 2 * layers * span == LANES
    table = []
    for layer in range(layers):
        for field in range(fields):
            high, low = widths(field, layer)
            table.append((field, layer, high, low, slot(field) + layer * span))
    return table


def fine_slot(field):
    if field < Q:
        return 4 * field
    if field in (MU, LAM):
        return 12 + 2 * (field - MU)
    return LANES // 2 + {W: 0, Q: 2, Q + 1: 4, Q + 2: 6, RHO: 8}[field]


def coarse_slot(field):
    if field < Q:
        return 2 * field
    return 6 if field == MU else LANES // 2 + {LAM: 0, Q: 2, Q + 1: 3, Q + 2: 4, RHO: 5}[field]


def round_up(value, multiple):
    return -(-value // multiple) * multiple


FINE_SPAN, COARSE_SPAN = 16, 8


def tables(fine_layers, coarse_layers):
    fine = plane_table(
        FINE_FIELDS, fine_layers, lambda f, l: fine_widths(f, l, fine_layers), fine_slot, FINE_SPAN
    )
    coarse = plane_table(
        COARSE_FIELDS, coarse_layers, lambda f, l: coarse_widths(f), coarse_slot, COARSE_SPAN
    )
    return fine, coarse


def edge_rows(tables_of_grids, parts_of_grids, first):
    pieces, at = [], 0
    for grid, (table, parts) in enumerate(zip(tables_of_grids, parts_of_grids)):
        for field, layer, high, low, _ in table:
            size = high if first else low
            for t in range(parts):
                pieces.append((grid, field, layer, t, size, at))
                at += size
    return pieces, round_up(at, 8)


def grid_tables(fine_shape, coarse_shape):
    fine, coarse = tables(fine_shape[1], coarse_shape[1])
    return (fine, coarse), (fine_shape[3] // LANES, coarse_shape[3] // LANES)


def pack_x_kernel(fu, fp, fm, cu, cp, cm, fine, coarse, to_even, to_odd, sems):
    copies = []
    for out, sources in ((fine, (fu, fp, fm)), (coarse, (cu, cp, cm))):
        for first, source in zip((U, Q, RHO), sources):
            copies.append(
                pltpu.make_async_copy(
                    source, out.at[first : first + source.shape[0]], sems.at[len(copies)]
                )
            )
    for copy in copies:
        copy.start()
    for copy in copies:
        copy.wait()
    grids = grid_tables(fine.shape, coarse.shape)

    def fill(out, first):
        for grid, field, layer, t, size, at in edge_rows(*grids, first)[0]:
            ref = (fine, coarse)[grid]
            start = 0 if first else ref.shape[2] - size
            out[at : at + size, :] = ref[
                field, layer, start : start + size, t * LANES : (t + 1) * LANES
            ]

    even = lax.rem(lax.axis_index("gx"), 2) == 0

    @pl.when(even)
    def _():
        fill(to_even, False)
        fill(to_odd, True)

    @pl.when(jnp.logical_not(even))
    def _():
        fill(to_even, True)
        fill(to_odd, False)


class Bundle:
    def __init__(self, fine_shape, coarse_shape):
        self.layers = fine_shape[1], coarse_shape[1]
        self.parts = fine_shape[3] // LANES, coarse_shape[3] // LANES
        self.rows = fine_shape[2] // 8, coarse_shape[2] // 8
        self.halo_base, self.ends_base, self.inner_base, at, inner = [], [], [], 0, 0
        for grid, fields in enumerate((FINE_FIELDS, COARSE_FIELDS)):
            self.halo_base.append(at)
            at += fields * self.layers[grid] * self.parts[grid]
            self.ends_base.append(at)
            at += fields
            self.inner_base.append(inner)
            inner += fields * self.rows[grid]
        self.size, self.inner_size = at, inner
        self.halo_fields = FINE_FIELDS, COARSE_FIELDS

    def halo(self, grid, field, layer, part):
        return self.halo_base[grid] + (field * self.layers[grid] + layer) * self.parts[grid] + part

    def inner(self, grid, field, row):
        return self.inner_base[grid] + field * self.rows[grid] + row

    def ends(self, inner, tiles, grid, field):
        own = [inner[self.inner(grid, field, r)] for r in range(self.rows[grid])]
        return jnp.concatenate(own + [tiles[self.ends_base[grid] + field]], axis=0)


def end_columns(read, layers, span):
    for layer in range(layers):
        first, last = read(layer)
        lane = lax.broadcasted_iota(jnp.int32, first.shape, 1)
        value = jnp.where(lane < LANES // 2, first, last)
        value = pltpu.roll(value, layer * span + span // 2, 1)
        total = value if layer == 0 else jnp.where(lane >= layer * span, value, total)
    return total


def packed_columns(table, ends_of, span):
    sides = [[None, None], [None, None]]
    for field, layer, high, low, slot in sorted(table, key=lambda entry: entry[4]):
        if layer:
            continue
        ends = ends_of(field)
        lane = lax.broadcasted_iota(jnp.int32, ends.shape, 1)
        within = jnp.bitwise_and(lane, span - 1)
        half, start = divmod(slot, LANES // 2)
        for side, first in enumerate((span // 2, span // 2 - low)):
            shift = (slot - first) % LANES
            value = pltpu.roll(ends, shift, 1) if shift else ends
            before = sides[side][half]
            sides[side][half] = (
                value if before is None else jnp.where(within >= start, value, before)
            )
    return [jnp.where(lane < LANES // 2, lower, upper) for lower, upper in sides]


SPANS = FINE_SPAN, COARSE_SPAN


def pack_inner_kernel(bundle, fine, coarse, inner, firsts_ref, lasts_ref):
    at = 0
    for grid, (table, ref) in enumerate(zip(tables(*bundle.layers), (fine, coarse))):
        fields = []
        for field in range(ref.shape[0]):

            def read(layer):
                return ref[field, layer, :, :LANES], ref[field, layer, :, ref.shape[3] - LANES :]

            ends = end_columns(read, ref.shape[1], SPANS[grid])
            fields.append(ends)
            for r in range(bundle.rows[grid]):
                inner[bundle.inner(grid, field, r)] = ends[r * 8 : (r + 1) * 8]
        rows = slice(at, at + ref.shape[2])
        firsts_ref[rows, :], lasts_ref[rows, :] = packed_columns(
            table, lambda field: fields[field], SPANS[grid]
        )
        at += ref.shape[2]


def pack_y_kernel(bundle, firsts_ref, lasts_ref, got_even, got_odd, out, to_even, to_odd):
    grids = tables(*bundle.layers), bundle.parts

    def halo(high_ref, low_ref):
        for first, ref in ((True, high_ref), (False, low_ref)):
            for grid, field, layer, t, size, at in edge_rows(*grids, first)[0]:
                start = 0 if first else MARGIN - size
                out[bundle.halo(grid, field, layer, t), start : start + size, :] = ref[
                    at : at + size, :
                ]

    for grid, table in enumerate(grids[0]):
        for field, layer, *_ in table:
            for t in range(bundle.parts[grid] if field < Q else 0):
                out[bundle.halo(grid, field, layer, t)] = jnp.zeros((MARGIN, LANES), jnp.float32)

    even = lax.rem(lax.axis_index("gx"), 2) == 0

    @pl.when(even)
    def _():
        halo(got_even, got_odd)

    @pl.when(jnp.logical_not(even))
    def _():
        halo(got_odd, got_even)

    packed, at = [], 0
    for grid, table in enumerate(grids[0]):
        fields = []
        for field in range(bundle.halo_fields[grid]):

            def read(layer):
                parts = (0, bundle.parts[grid] - 1)
                return [out[bundle.halo(grid, field, layer, t)] for t in parts]

            ends = end_columns(read, bundle.layers[grid], SPANS[grid])
            fields.append(ends)
            out[bundle.ends_base[grid] + field] = ends
        columns = packed_columns(table, lambda field: fields[field], SPANS[grid])
        rows = slice(at, at + 8 * bundle.rows[grid])
        packed.append((rows, columns))
        at = rows.stop
    even_y = lax.rem(lax.axis_index("gy"), 2) == 0

    def place(first_out, last_out):
        at = 0
        for rows, (firsts, lasts) in packed:
            size = rows.stop - rows.start
            first_out[at : at + size, :] = firsts_ref[rows, :]
            last_out[at : at + size, :] = lasts_ref[rows, :]
            first_out[at + size : at + size + MARGIN, :] = firsts
            last_out[at + size : at + size + MARGIN, :] = lasts
            at += size + MARGIN

    @pl.when(even_y)
    def _():
        place(to_odd, to_even)

    @pl.when(jnp.logical_not(even_y))
    def _():
        place(to_even, to_odd)


def ahead(value, axis):
    return pltpu.roll(value, value.shape[axis] - 1, axis)


def behind(value, axis):
    return value - pltpu.roll(value, 1, axis)


def stress_of(here, below, medium, stretched):
    rigidity, lame = medium[0], medium[1]
    dx = [ahead(f, 0) - f for f in here]
    dy = [ahead(f, 1) - f for f in here]
    dz = [b - f for b, f in zip(below, here)]
    if stretched:
        dz = [f * medium[2] for f in dz]
    trace = lame * (dx[0] + dy[1] + dz[2])
    double = rigidity + rigidity
    return (
        trace + double * dx[0],
        trace + double * dy[1],
        trace + double * dz[2],
        rigidity * (dy[0] + dx[1]),
        rigidity * (dz[0] + dx[2]),
        rigidity * (dz[1] + dy[2]),
    )


def force_of(stress, above, outward):
    nx, ny, nz, xy, xz, yz = stress
    up = [xz, yz, nz]
    if above is not None:
        up = [f - a for f, a in zip(up, (above[4], above[5], above[2]))]
    if outward is not None:
        up = [f * outward for f in up]
    return (
        behind(nx, 0) + behind(xy, 1) + up[0],
        behind(xy, 0) + behind(ny, 1) + up[1],
        behind(xz, 0) + behind(yz, 1) + up[2],
    )


def bf16_parts(value):
    parts = []
    for _ in range(3):
        part = value.astype(jnp.bfloat16)
        parts.append(part)
        value = value - part.astype(jnp.float32)
    return parts


def select_lanes(planes, matrix):
    rows = planes[0].shape[0]
    parts = bf16_parts(jnp.concatenate(planes, axis=0))
    product = jnp.dot(
        jnp.concatenate(parts, axis=0), matrix, preferred_element_type=jnp.float32
    )
    size = rows * len(planes)
    total = product[:size] + product[size : 2 * size] + product[2 * size :]
    return [total[k * rows : (k + 1) * rows] for k in range(len(planes))]


def select_rows(matrix, planes):
    lanes = planes[0].shape[1]
    parts = bf16_parts(jnp.concatenate(planes, axis=1))
    product = jnp.dot(
        jnp.concatenate([matrix] * 3, axis=1),
        jnp.concatenate(parts, axis=0),
        preferred_element_type=jnp.float32,
    )
    return [product[:, k * lanes : (k + 1) * lanes] for k in range(len(planes))]


def bf16_mask(condition):
    return jnp.where(condition, 1.0, 0.0).astype(jnp.bfloat16)


class Grids:
    def __init__(self, height, cheight, lanes, clanes, lane_of):
        def pairs(shape, fine_axis, size_of):
            f = lax.broadcasted_iota(jnp.int32, shape, fine_axis)
            c = lax.broadcasted_iota(jnp.int32, shape, 1 - fine_axis)
            return bf16_mask(size_of(f) == c)

        def row_of(f):
            turn = height - MARGIN // 2
            return jnp.right_shift(jnp.where(f < turn, f, f - height + 2 * cheight), 1)

        self.up_rows = pairs((height, cheight), 0, row_of)
        self.down_rows = pairs((cheight, height), 1, row_of)
        self.up_lanes = pairs((clanes, lanes), 1, lane_of)
        self.down_lanes = pairs((lanes, clanes), 0, lane_of)

    def prolong(self, planes):
        return select_rows(self.up_rows, select_lanes(planes, self.up_lanes))

    def restrict(self, planes):
        planes = select_lanes(select_rows(self.down_rows, planes), self.down_lanes)
        return [0.25 * plane for plane in planes]


def row_index(height, shape):
    index = lax.broadcasted_iota(jnp.int32, shape, 0)
    return jnp.where(index < height - MARGIN // 2, index, index - height)


def solver(plane, medium, ghost_above, ghost_below, last, stretched):
    known = {}

    def here(g):
        if g < 0:
            return ghost_above
        if g == last + 1:
            return ghost_below
        return [plane(k, g) for k in range(3)]

    def stress(g):
        if g < 0 and ghost_above is None:
            return None
        if g not in known:
            fields = (MU, LAM, W) if stretched else (MU, LAM)
            known[g] = stress_of(
                here(g), here(g + 1), [medium(k, max(g, 0)) for k in fields], stretched
            )
        return known[g]

    return stress


def advance(plane, before, medium, stress, g, scale, stretched):
    force = force_of(stress(g), stress(g - 1), medium(W, g) if stretched else None)
    rate = scale / medium(RHO, g)
    return [
        plane(k, g) + plane(k, g) - before(k, g) + force[k] * rate for k in range(3)
    ]


def step_scales():
    scale = jnp.float32(time_step * time_step)
    return scale, 0.25 * scale


def first_step(dev, layers, clayers, fine, coarse, grids, keep_f, keep_c, state_f, state_c):
    depth, cdepth = 2 * layers, 2 * clayers
    scale, cscale = step_scales()
    three = range(3)
    ghost_f = grids.prolong([coarse(k, 0) for k in three])
    ghost_c = grids.restrict([fine(k, depth - 1) for k in three])
    zero_c = [jnp.zeros_like(ghost_c[0])] * 3
    stress_f = solver(fine, fine, None, ghost_f, depth - 1, True)
    stress_c = solver(coarse, coarse, ghost_c, zero_c, cdepth - 1, False)
    near = {*range(max(dev * layers - 1, 0), min((dev + 1) * layers + 1, depth)), depth - 1}
    cnear = {0, *range(max(dev * clayers - 1, 0), min((dev + 1) * clayers + 1, cdepth))}
    for g in sorted(near):
        values = advance(fine, lambda k, g: fine(Q + k, g), fine, stress_f, g, scale, True)
        for k in three:
            state_f[k, g] = jnp.where(keep_f(g), values[k], 0.0)
    for g in sorted(cnear):
        values = advance(coarse, lambda k, g: coarse(Q + k, g), coarse, stress_c, g, cscale, False)
        for k in three:
            state_c[k, g] = jnp.where(keep_c, values[k], 0.0)


def second_step(dev, layers, clayers, fine, coarse, grids, state_f, state_c, out_f, out_c):
    depth, cdepth = 2 * layers, 2 * clayers
    scale, cscale = step_scales()
    ghost_f = ghost_c = None
    if dev == 1:
        ghost_f = grids.prolong([state_c[k, 0] for k in range(3)])
    else:
        ghost_c = grids.restrict([state_f[k, depth - 1] for k in range(3)])
    zero_c = [jnp.zeros(state_c.shape[2:], jnp.float32)] * 3
    now_f, now_c = lambda k, g: state_f[k, g], lambda k, g: state_c[k, g]
    stress_f = solver(now_f, fine, None, ghost_f, depth - 1, True)
    stress_c = solver(now_c, coarse, ghost_c, zero_c, cdepth - 1, False)
    for l in range(layers):
        values = advance(now_f, fine, fine, stress_f, dev * layers + l, scale, True)
        for k in range(3):
            out_f[k, l] = values[k][: out_f.shape[2]]
    for l in range(clayers):
        values = advance(now_c, coarse, coarse, stress_c, dev * clayers + l, cscale, False)
        for k in range(3):
            out_c[k, l] = values[k][: out_c.shape[2]]


def for_each_core(body):
    dev = lax.axis_index("dev")

    @pl.when(dev == 0)
    def _():
        body(0)

    @pl.when(dev != 0)
    def _():
        body(1)


def inside(index, axis, size):
    at = index + lax.axis_index(axis) * size
    return (at >= 0) & (at < lax.axis_size(axis) * size)


def readers(dev, bundle, own_f, own_c, far_f, far_c, own_b, far_b):
    def reader(grid, own, far):
        def read(field, g):
            layer = g % bundle.layers[grid]
            mine = g // bundle.layers[grid] == dev
            ref, tiles = (own, own_b) if mine else (far, far_b)
            halo = [
                tiles[bundle.halo(grid, field, layer, t)] for t in range(bundle.parts[grid])
            ]
            return jnp.concatenate([ref[field, layer], jnp.concatenate(halo, axis=1)], axis=0)

        return read

    return reader(0, own_f, far_f), reader(1, own_c, far_c)


def tile_grids(own_f, own_c):
    return Grids(
        own_f.shape[2] + MARGIN, own_c.shape[2] + MARGIN, own_f.shape[3], own_c.shape[3],
        lambda f: jnp.right_shift(f, 1),
    )


def first_kernel(bundle, own_f, own_c, far_f, far_c, own_b, far_b, state_f, state_c):
    _, layers, n, width = own_f.shape
    _, clayers, nc, cwidth = own_c.shape
    fx = row_index(n + MARGIN, (n + MARGIN, width))
    cx = row_index(nc + MARGIN, (nc + MARGIN, cwidth))
    rows_f = inside(fx, "gx", n) & (fx >= -1)
    keep_c = inside(cx, "gx", nc) & (cx >= -1) & (cx <= nc)
    grids = tile_grids(own_f, own_c)

    def body(dev):
        fine, coarse = readers(dev, bundle, own_f, own_c, far_f, far_c, own_b, far_b)
        first_step(
            dev, layers, clayers, fine, coarse, grids,
            lambda g: rows_f & (fx <= n + (g == 2 * layers - 1)), keep_c, state_f, state_c,
        )

    for_each_core(body)


def second_kernel(
    bundle, own_f, own_c, far_f, far_c, own_b, far_b, own_i, far_i, state_f, state_c,
    out_f, out_c, strip_f, strip_c,
):
    grids = tile_grids(own_f, own_c)

    def body(dev):
        fine, coarse = readers(dev, bundle, own_f, own_c, far_f, far_c, own_b, far_b)
        second_step(
            dev, own_f.shape[1], own_c.shape[1], fine, coarse, grids, state_f, state_c, out_f, out_c
        )

    for_each_core(body)
    top = lax.axis_index("dev") == 0
    for grid, (strip, span) in enumerate(((strip_f, FINE_SPAN), (strip_c, COARSE_SPAN))):
        lane = lax.broadcasted_iota(jnp.int32, (strip.shape[1], LANES), 1)
        for field in range(strip.shape[0]):
            own = bundle.ends(own_i, own_b, grid, field)
            far = bundle.ends(far_i, far_b, grid, field)
            upper, lower = jnp.where(top, own, far), jnp.where(top, far, own)
            whole = jnp.where(lane < LANES // 2, upper, pltpu.roll(lower, LANES // 2, 1))
            strip[field, :, :LANES] = pltpu.roll(whole, LANES - span // 4, 1)
            strip[field, :, LANES:] = whole


def strip_kernel(
    strip_f, strip_c, main_f, main_c, own_ye, own_yo, far_ye, far_yo, out_f, out_c,
    stage_f, stage_c, sems,
):
    layers, n, width = main_f.shape[1:]
    clayers, nc, cwidth = main_c.shape[1:]
    height, cheight = n + MARGIN, nc + MARGIN
    depth, cdepth = 2 * layers, 2 * clayers
    fine_table, coarse_table = tables(layers, clayers)
    three = range(3)
    top = lax.axis_index("dev") == 0
    even = lax.rem(lax.axis_index("gy"), 2) == 0
    wide = 2 * LANES

    def places(rows, span, extent):
        lane = lax.broadcasted_iota(jnp.int32, (rows, wide), 1)
        low = lane < LANES
        inner = jnp.bitwise_and(lane, LANES - 1)
        within = jnp.bitwise_and(lane, span - 1)
        room = span // 4
        at = jnp.where(low, within - room, within + extent - span // 2)
        used = within < span - room
        return jnp.right_shift(inner, span.bit_length() - 1), at, used

    fg, fy, used_f = places(height, FINE_SPAN, width)
    cg, cy, used_c = places(cheight, COARSE_SPAN, cwidth)
    fx, cx = row_index(height, (height, wide)), row_index(cheight, (cheight, wide))
    last = (fg == depth - 1).astype(jnp.int32)
    keep_f = (
        used_f & inside(fx, "gx", n) & inside(fy, "gy", width)
        & (fx >= -1) & (fy >= -1) & (fx <= n + last) & (fy <= width + last)
    )
    keep_c = (
        used_c & inside(cx, "gx", nc) & inside(cy, "gy", cwidth)
        & (cx >= -1) & (cx <= nc) & (cy >= -1) & (cy <= cwidth)
    )

    def filled(table, src, start, span):
        rows = src.shape[1]
        room = span // 4
        lane = lax.broadcasted_iota(jnp.int32, (rows, LANES), 1)
        within = jnp.bitwise_and(lane, span - 1)
        sides = []
        for e, o in ((own_ye, own_yo), (far_ye, far_yo)):
            e, o = e[start : start + rows, :], o[start : start + rows, :]
            sides.append((jnp.where(even, o, e), jnp.where(even, e, o)))
        uppers = [jnp.where(top, a, b) for a, b in zip(*sides)]
        lowers = [jnp.where(top, b, a) for a, b in zip(*sides)]
        fields = []
        for field in range(src.shape[0]):
            entries = [entry for entry in table if entry[0] == field]
            slot = entries[0][4]
            width_of = (max(e[3] for e in entries), max(e[2] for e in entries))
            parts = []
            for side in range(2):
                size = width_of[side]
                first = span // 2 if side else room - size
                shift = (first - slot) % LANES
                halo = jnp.where(
                    lane < LANES // 2,
                    pltpu.roll(uppers[side], shift, 1) if shift else uppers[side],
                    pltpu.roll(lowers[side], (shift + LANES // 2) % LANES, 1),
                )
                parts.append(
                    jnp.where(
                        (within >= first) & (within < first + size),
                        halo,
                        src[field, :, side * LANES : (side + 1) * LANES],
                    )
                )
            fields.append(jnp.concatenate(parts, axis=1))
        return fields

    fine = filled(fine_table, strip_f, 0, FINE_SPAN)
    coarse = filled(coarse_table, strip_c, height, COARSE_SPAN)

    def gather(value, index, axis):
        return jnp.take_along_axis(value, index, axis=axis)

    row = lax.broadcasted_iota(jnp.int32, (8, LANES), 0)
    lane = lax.broadcasted_iota(jnp.int32, (8, LANES), 1)
    bottom = (depth - 1) * FINE_SPAN
    up_lane = jnp.right_shift(jnp.maximum(lane - bottom, 0), 1)
    down_lane = jnp.minimum(lane * 2 + bottom, LANES - 2)

    def blocks(plane):
        return [
            [plane[r : r + 8, t : t + LANES] for r in range(0, plane.shape[0], 8)]
            for t in range(0, wide, LANES)
        ]

    def joined(tiles):
        return jnp.concatenate([jnp.concatenate(column, axis=0) for column in tiles], axis=1)

    def prolong(plane):
        tiles = []
        for column in blocks(plane):
            column = [gather(block, up_lane, 1) for block in column]
            out = [
                gather(column[b // 2], jnp.right_shift(row, 1) + 4 * (b % 2), 0)
                for b in range(n // 8)
            ]
            edge = jnp.right_shift(row, 1) + jnp.where(row < 4, 0, 4)
            tiles.append(out + [gather(column[-1], edge, 0)])
        return joined(tiles)

    def restrict(plane):
        def pair_rows(block, index):
            return gather(block, index, 0) + gather(block, index + 1, 0)

        tiles = []
        for column in blocks(plane):
            column = [gather(f, down_lane, 1) + gather(f, down_lane + 1, 1) for f in column]
            low, high = jnp.minimum(row * 2, 6), jnp.maximum(row * 2 - 8, 0)
            out = [
                jnp.where(row < 4, pair_rows(column[2 * b], low), pair_rows(column[2 * b + 1], high))
                for b in range(nc // 8)
            ]
            edge = jnp.where(row < 2, row * 2, jnp.maximum(row * 2 - 8, 0))
            tiles.append(out + [pair_rows(column[-1], edge)])
        return 0.25 * joined(tiles)

    scale = jnp.float32(time_step * time_step)

    def shifted(value, lanes):
        return pltpu.roll(value, lanes % wide, 1)

    def lift(stress, lanes, at_top, above):
        return [jnp.where(at_top, a, shifted(stress[k], lanes)) for k, a in zip((2, 4, 5), above)]

    def step(u, p, v, q):
        ghost_f = [prolong(f) for f in v]
        ghost_c = [restrict(f) for f in u]
        below = [jnp.where(fg == depth - 1, b, shifted(f, -FINE_SPAN)) for f, b in zip(u, ghost_f)]
        stress = stress_of(u, below, [fine[k] for k in (MU, LAM, W)], True)
        up = lift(stress, FINE_SPAN, fg == 0, [0.0] * 3)
        force = force_of(stress, {2: up[0], 4: up[1], 5: up[2]}, fine[W])
        rate = scale / fine[RHO]
        next_u = [a + a - b + f * rate for a, b, f in zip(u, p, force)]
        medium = [coarse[k] for k in (MU, LAM)]
        under = [jnp.where(cg == cdepth - 1, 0.0, shifted(f, -COARSE_SPAN)) for f in v]
        stress = stress_of(v, under, medium, False)
        above = stress_of(ghost_c, v, medium, False)
        up = lift(stress, COARSE_SPAN, cg == 0, [above[k] for k in (2, 4, 5)])
        force = force_of(stress, {2: up[0], 4: up[1], 5: up[2]}, None)
        rate = (0.25 * scale) / coarse[RHO]
        next_v = [a + a - b + f * rate for a, b, f in zip(v, q, force)]
        return next_u, next_v

    u, v = fine[:3], coarse[:3]
    next_u, next_v = step(u, fine[Q:RHO], v, coarse[Q:RHO])
    next_u = [jnp.where(keep_f, f, 0.0) for f in next_u]
    next_v = [jnp.where(keep_c, f, 0.0) for f in next_v]
    last_u, last_v = step(next_u, u, next_v, v)

    copies = []
    for values, result, out, main, span in (
        (last_u, out_f, stage_f, main_f, FINE_SPAN),
        (last_v, out_c, stage_c, main_c, COARSE_SPAN),
    ):
        cells, extent = out.shape[2:]
        room = span // 4
        lane = lax.broadcasted_iota(jnp.int32, (cells, LANES), 1)
        for k in three:
            ends = [values[k][:cells, side * LANES : (side + 1) * LANES] for side in range(2)]
            ends = [jnp.where(top, e, pltpu.roll(e, LANES // 2, 1)) for e in ends]
            for l in range(out.shape[1]):
                first = pltpu.roll(ends[0], LANES - l * span - room, 1)
                final = pltpu.roll(ends[1], LANES - l * span - span // 2, 1)
                for start in range(0, extent, LANES):
                    part = main[k, l, :, start : start + LANES]
                    if start == 0:
                        part = jnp.where(lane < room, first, part)
                    if start == extent - LANES:
                        part = jnp.where(lane >= LANES - room, final, part)
                    out[k, l, :, start : start + LANES] = part
            copies.append(pltpu.make_async_copy(out.at[k], result.at[k], sems.at[len(copies)]))
            copies[-1].start()
    for copy in copies:
        copy.wait()


def partners(count, parity):
    pairs = [(i, ((i + parity) ^ 1) - parity) for i in range(count)]
    return [(i, j) for i, j in pairs if 0 <= j < count]


def swap(value, axis, parity):
    return lax.ppermute(value, axis, partners(lax.axis_size(axis), parity))


def call(
    kernel, out_shape, operands, scratch=(), flops=0, space=pltpu.VMEM, to=pltpu.VMEM, limit=24
):
    size = sum(o.size for o in out_shape) * 4
    call = pl.pallas_call(
        kernel,
        out_shape=out_shape,
        in_specs=[pl.BlockSpec(memory_space=space)] * len(operands),
        out_specs=[pl.BlockSpec(memory_space=to)] * len(out_shape),
        scratch_shapes=list(scratch),
        cost_estimate=pl.CostEstimate(flops=flops, bytes_accessed=size, transcendentals=0),
        compiler_params=pltpu.CompilerParams(vmem_limit_bytes=limit * 1024 * 1024),
    )
    if space == pltpu.HBM:
        operands = [pltpu.with_memory_space_constraint(o, space) for o in operands]
    return call(*operands)


def shape(*dims):
    return jax.ShapeDtypeStruct(dims, jnp.float32)


def per_device(*inputs):
    _, layers, n, width = inputs[0].shape
    _, clayers, nc, cwidth = inputs[3].shape
    grids = grid_tables(inputs[0].shape, inputs[3].shape)
    rows = max(edge_rows(*grids, first)[1] for first in (True, False))
    height, cheight = n + MARGIN, nc + MARGIN

    edge = shape(rows, LANES)
    own_f, own_c, to_even, to_odd = call(
        pack_x_kernel,
        (shape(FINE_FIELDS, layers, n, width), shape(COARSE_FIELDS, clayers, nc, cwidth), edge, edge),
        inputs,
        scratch=(pltpu.SemaphoreType.DMA((6,)),),
        space=pltpu.HBM,
        limit=24,
    )
    got_odd = swap(to_odd, "gx", 1)
    got_even = swap(to_even, "gx", 0)
    far_f, far_c = swap(own_f, "dev", 0), swap(own_c, "dev", 0)

    bundle = Bundle(inputs[0].shape, inputs[3].shape)
    inner = shape(n + nc, LANES)
    own_i, firsts, lasts = call(
        functools.partial(pack_inner_kernel, bundle),
        (shape(bundle.inner_size, 8, LANES), inner, inner),
        (own_f, own_c),
    )
    far_i = swap(own_i, "dev", 0)

    side = shape(height + cheight, LANES)
    own_b, to_even, to_odd = call(
        functools.partial(pack_y_kernel, bundle),
        (shape(bundle.size, 8, LANES), side, side),
        (firsts, lasts, got_even, got_odd),
    )
    own_yo = swap(to_odd, "gy", 1)
    own_ye = swap(to_even, "gy", 0)
    far_b = swap(own_b, "dev", 0)

    tiles = (own_f, own_c, far_f, far_c, own_b, far_b)
    states = call(
        functools.partial(first_kernel, bundle),
        (shape(3, 2 * layers, height, width), shape(3, 2 * clayers, cheight, cwidth)),
        tiles,
        flops=STEP_FLOPS,
    )
    results = (shape(*inputs[0].shape), shape(*inputs[3].shape))
    strips = (
        shape(FINE_FIELDS, height, 2 * LANES),
        shape(COARSE_FIELDS, cheight, 2 * LANES),
    )
    main_f, main_c, strip_f, strip_c = call(
        functools.partial(second_kernel, bundle),
        results + strips,
        tiles + (own_i, far_i) + tuple(states),
        flops=STEP_FLOPS,
    )
    far_yo, far_ye = swap(own_yo, "dev", 0), swap(own_ye, "dev", 0)
    return call(
        strip_kernel,
        results,
        (strip_f, strip_c, main_f, main_c, own_ye, own_yo, far_ye, far_yo),
        scratch=tuple(pltpu.VMEM(r.shape, jnp.float32) for r in results)
        + (pltpu.SemaphoreType.DMA((6,)),),
        to=pltpu.HBM,
    )


STEP_FLOPS = 2_000_000


def solution(mesh):
    spec = P(None, "dev", "gx", "gy")

    return jax.shard_map(
        per_device,
        mesh=mesh,
        in_specs=(spec,) * 6,
        out_specs=(spec, spec),
        check_vma=False,
    )
```
